32 devices in a mesh: dp: 1 (over z), tp: 4 (over y), sq: 8 (over x, core).
Axes of the slice: x: 4, y: 4, z: 1, core: 2. Of those that a mesh axis runs over, the one named last changes fastest.
The devices are a block of a 4x4x8 slice.
Arguments:
- x_steps: bfloat16 [4, 32, 6144], P(None, 'dp')
- positions: int32 [32], P('dp')
- k_cache: bfloat16 [32, 4096, 4, 128], P('dp', 'sq', 'tp')
- v_cache: bfloat16 [32, 4096, 4, 128], P('dp', 'sq', 'tp')
- w_q: bfloat16 [6144, 6144], P(None, 'tp')
- b_q: bfloat16 [6144], P('tp')
- w_k: bfloat16 [6144, 512], P(None, 'tp')
- b_k: bfloat16 [512], P('tp')
- w_v: bfloat16 [6144, 512], P(None, 'tp')
- b_v: bfloat16 [512], P('tp')
- w_o: bfloat16 [6144, 6144], P('tp')
- b_o: bfloat16 [6144], replicated
- ln1_gain: bfloat16 [6144], replicated
- ln1_bias: bfloat16 [6144], replicated
- ln2_gain: bfloat16 [6144], replicated
- ln2_bias: bfloat16 [6144], replicated
- w_fc: bfloat16 [6144, 24576], P(None, 'tp')
- b_fc: bfloat16 [24576], P('tp')
- w_proj: bfloat16 [24576, 6144], P('tp')
- b_proj: bfloat16 [6144], replicated
Outputs:
- output 1: bfloat16 [4, 32, 6144], P(None, 'dp')
- output 2: bfloat16 [32, 4096, 4, 128], P('dp', 'sq', 'tp')
- output 3: bfloat16 [32, 4096, 4, 128], P('dp', 'sq', 'tp')
All inputs are finite; a program needn't handle non-finite values.
Results may differ from the reference program's by a relative error of at most 0.0152474.
Values sent between devices are 32-bit elements.
A program may use at most 768 MiB of HBM per device.

```python
import jax
import jax.numpy as jnp
from jax import lax

D = 6144
HEADS = 48
KV_HEADS = 4
HEAD = 128
FF = 24576
WINDOW = 4096
BATCH = 32
STEPS = 4
ROPE_BASE = 1000000
POS_LOW = 100
POS_HIGH = 15000
HOT_ODDS = 512
HOT_RUN = 8


def rope_tables(positions, head_dim):
    half_dim = head_dim // 2
    inv_freq = jnp.power(jnp.float32(ROPE_BASE), -2.0 * jnp.arange(half_dim, dtype=jnp.float32) / head_dim)
    angle = positions.astype(jnp.float32)[..., None] * inv_freq
    return jnp.cos(angle), jnp.sin(angle)


def apply_rope(vectors, cos_t, sin_t):
    half_dim = vectors.shape[-1] // 2
    first = vectors[..., :half_dim]
    second = vectors[..., half_dim:]
    return jnp.concatenate([first * cos_t - second * sin_t, second * cos_t + first * sin_t], axis=-1)


def layer_norm(vectors, gain, shift):
    row_mean = jnp.mean(vectors, axis=-1, keepdims=True)
    centered = vectors - row_mean
    row_var = jnp.mean(centered * centered, axis=-1, keepdims=True)
    return centered * lax.rsqrt(row_var + 1e-5) * gain.astype(jnp.float32) + shift.astype(jnp.float32)


def linear(rows_in, weight, bias):
    return jnp.dot(rows_in, weight, preferred_element_type=jnp.float32) + bias.astype(jnp.float32)


def hot_direction():
    dim_ids = jnp.arange(HEAD)
    marked = (dim_ids % (HEAD // 2)) >= HEAD // 2 - 4
    return jnp.where(marked, 8.0 ** -0.5, 0.0).astype(jnp.float32)


def draw_positions(key):
    key_low, key_high, key_pick, key_perm = jax.random.split(key, 4)
    short = jax.random.randint(key_low, (BATCH,), POS_LOW, WINDOW)
    longer = jax.random.randint(key_high, (BATCH,), WINDOW, POS_HIGH + 1)
    chooser = jax.random.randint(key_pick, (BATCH,), 0, 4)
    mixed = jnp.where(chooser == 0, short, longer)
    mixed = mixed.at[0].set(POS_LOW).at[1].set(POS_HIGH)
    return jax.random.permutation(key_perm, mixed).astype(jnp.int32)


def setup_inputs(seed: int = 0, part: int = 0) -> dict:
    shared = jax.random.split(jax.random.key(seed), 16)
    own = jax.random.split(jax.random.fold_in(jax.random.key(seed + 1), part), 5)
    hot_amp = (8.0 * HEAD ** 0.5) ** 0.5
    hot_vec = hot_direction() * hot_amp
    positions = draw_positions(own[0])
    slot_ids = jnp.arange(WINDOW, dtype=jnp.int32)
    last_pos = positions[:, None] - 1
    held_pos = last_pos - (last_pos - slot_ids[None, :]) % WINDOW
    hot_slot = (jax.random.randint(own[1], (BATCH, WINDOW), 0, HOT_ODDS) == 0) | ((slot_ids[None, :] - positions[:, None]) % WINDOW < HOT_RUN)
    cos_t, sin_t = rope_tables(held_pos, HEAD)
    hot_keys = apply_rope(jnp.broadcast_to(hot_vec, (BATCH, WINDOW, HEAD)), cos_t, sin_t)
    hot_keys = jnp.where(hot_slot[:, :, None], hot_keys, 0.0)
    k_cache = (jax.random.normal(own[2], (BATCH, WINDOW, KV_HEADS, HEAD), jnp.float32) + hot_keys[:, :, None, :]).astype(jnp.bfloat16)
    v_cache = jax.random.normal(own[3], (BATCH, WINDOW, KV_HEADS, HEAD), jnp.float32).astype(jnp.bfloat16)
    x_steps = jax.random.normal(own[4], (STEPS, BATCH, D), jnp.float32).astype(jnp.bfloat16)

    def scaled(key, shape, scale):
        return (jax.random.normal(key, shape, jnp.float32) * scale).astype(jnp.bfloat16)

    b_q = (0.5 * jax.random.normal(shared[1], (HEADS * HEAD,), jnp.float32) + jnp.tile(hot_vec, HEADS)).astype(jnp.bfloat16)
    b_k = (0.5 * jax.random.normal(shared[3], (KV_HEADS * HEAD,), jnp.float32) + jnp.tile(hot_vec, KV_HEADS)).astype(jnp.bfloat16)
    return {
        "x_steps": x_steps,
        "positions": positions,
        "k_cache": k_cache,
        "v_cache": v_cache,
        "w_q": scaled(shared[0], (D, HEADS * HEAD), D ** -0.5),
        "b_q": b_q,
        "w_k": scaled(shared[2], (D, KV_HEADS * HEAD), D ** -0.5),
        "b_k": b_k,
        "w_v": scaled(shared[4], (D, KV_HEADS * HEAD), D ** -0.5),
        "b_v": scaled(shared[5], (KV_HEADS * HEAD,), 0.5),
        "w_o": scaled(shared[6], (HEADS * HEAD, D), 3.0 * (HEADS * HEAD) ** -0.5),
        "b_o": scaled(shared[7], (D,), 0.2),
        "ln1_gain": (1.0 + 0.2 * jax.random.normal(shared[8], (D,), jnp.float32)).astype(jnp.bfloat16),
        "ln1_bias": scaled(shared[9], (D,), 0.2),
        "ln2_gain": (1.0 + 0.2 * jax.random.normal(shared[10], (D,), jnp.float32)).astype(jnp.bfloat16),
        "ln2_bias": scaled(shared[11], (D,), 0.2),
        "w_fc": scaled(shared[12], (D, FF), D ** -0.5),
        "b_fc": scaled(shared[13], (FF,), 0.5),
        "w_proj": scaled(shared[14], (FF, D), 1.5 * FF ** -0.5),
        "b_proj": scaled(shared[15], (D,), 0.2),
    }


def reference(x_steps, positions, k_cache, v_cache, w_q, b_q, w_k, b_k, w_v, b_v, w_o, b_o,
              ln1_gain, ln1_bias, ln2_gain, ln2_bias, w_fc, b_fc, w_proj, b_proj):
    group = HEADS // KV_HEADS
    slot_ids = jnp.arange(WINDOW, dtype=jnp.int32)
    batch_ids = jnp.arange(BATCH, dtype=jnp.int32)
    score_scale = HEAD ** -0.5

    def attend_one(packed):
        q_one, k_one, v_one, slot_ok = packed
        scores = jnp.einsum("grd,wgd->grw", q_one.reshape(KV_HEADS, group, HEAD).astype(jnp.float32), k_one.astype(jnp.float32)) * score_scale
        scores = jnp.where(slot_ok[None, None, :], scores, -1e30)
        weights = jax.nn.softmax(scores, axis=-1)
        return jnp.einsum("grw,wgd->grd", weights, v_one.astype(jnp.float32))

    def one_step(carry, step_in):
        key_buf, val_buf = carry
        x_in, step_idx = step_in
        cur_pos = positions + step_idx
        hidden = layer_norm(x_in.astype(jnp.float32), ln1_gain, ln1_bias).astype(jnp.bfloat16)
        query = linear(hidden, w_q, b_q).astype(jnp.bfloat16)
        key_new = linear(hidden, w_k, b_k).astype(jnp.bfloat16)
        val_new = linear(hidden, w_v, b_v).astype(jnp.bfloat16)
        cos_t, sin_t = rope_tables(cur_pos, HEAD)
        q_rot = apply_rope(query.reshape(BATCH, HEADS, HEAD).astype(jnp.float32), cos_t[:, None, :], sin_t[:, None, :]).astype(jnp.bfloat16)
        k_rot = apply_rope(key_new.reshape(BATCH, KV_HEADS, HEAD).astype(jnp.float32), cos_t[:, None, :], sin_t[:, None, :]).astype(jnp.bfloat16)
        write_slot = cur_pos % WINDOW
        key_buf = key_buf.at[batch_ids, write_slot].set(k_rot)
        val_buf = val_buf.at[batch_ids, write_slot].set(val_new.reshape(BATCH, KV_HEADS, HEAD))
        held_pos = cur_pos[:, None] - (cur_pos[:, None] - slot_ids[None, :]) % WINDOW
        attn = lax.map(attend_one, (q_rot, key_buf, val_buf, held_pos >= 0))
        attn_out = attn.astype(jnp.bfloat16).reshape(BATCH, HEADS * HEAD)
        x_mid = (x_in.astype(jnp.float32) + jnp.dot(attn_out, w_o, preferred_element_type=jnp.float32) + b_o.astype(jnp.float32)).astype(jnp.bfloat16)
        hidden_two = layer_norm(x_mid.astype(jnp.float32), ln2_gain, ln2_bias).astype(jnp.bfloat16)
        gelu_out = jax.nn.gelu(linear(hidden_two, w_fc, b_fc), approximate=True).astype(jnp.bfloat16)
        y_out = (x_mid.astype(jnp.float32) + jnp.dot(gelu_out, w_proj, preferred_element_type=jnp.float32) + b_proj.astype(jnp.float32)).astype(jnp.bfloat16)
        return (key_buf, val_buf), y_out

    (k_final, v_final), y_steps = lax.scan(one_step, (k_cache, v_cache), (x_steps, jnp.arange(STEPS, dtype=jnp.int32)))
    return y_steps, k_final, v_final
```

```python
import functools

import jax
import jax.numpy as jnp
from jax import lax
from jax.experimental import pallas as pl
from jax.experimental.pallas import tpu as pltpu
from jax.sharding import PartitionSpec as P

ROPE_BASE = 1000000.0
LN_EPS = 1e-5
NEG_BIG = -1e30
MESH = pl.DeviceIdType.MESH
F32 = jnp.float32
BF16 = jnp.bfloat16
VMEM_BYTES = 67043328


def one_hot_rows(size, inner):
    outer = size // inner
    row = lax.broadcasted_iota(jnp.int32, (size, size), 0)
    col = lax.broadcasted_iota(jnp.int32, (size, size), 1)
    source = lax.rem(row, outer) * inner + lax.div(row, outer)
    return jnp.where(col == source, 1.0, 0.0).astype(BF16)


def qkv_kernel(x_any, wq_any, wk_any, wv_any, bias_ref, vec_ref, cos_ref, sin_ref, out_ref,
               x_buf, w_buf, hid, x_sem, w_sem, *, batch, tiles, tile, head_dim):
    rows, width = x_buf.shape
    x_copy = pltpu.make_async_copy(x_any, x_buf, x_sem)
    x_copy.start()
    for t in range(tiles - 1):
        pltpu.make_async_copy(wq_any.at[:, pl.ds(t * tile, tile)], w_buf.at[t], w_sem.at[t]).start()
    k_copy = pltpu.make_async_copy(wk_any, w_buf.at[tiles - 1, :, pl.ds(0, head_dim)], w_sem.at[tiles - 1])
    v_copy = pltpu.make_async_copy(wv_any, w_buf.at[tiles - 1, :, pl.ds(head_dim, head_dim)], w_sem.at[tiles])
    k_copy.start()
    v_copy.start()
    x_copy.wait()
    gain = vec_ref[0:1, :]
    shift = vec_ref[1:2, :]

    def norm_rows(i, carry):
        at = pl.ds(pl.multiple_of(i * 16, 16), 16)
        vals = x_buf[at, :].astype(F32)
        mean = jnp.sum(vals, axis=-1, keepdims=True) * (1.0 / width)
        vals = vals - mean
        var = jnp.sum(vals * vals, axis=-1, keepdims=True) * (1.0 / width)
        hid[at, :] = (vals * lax.rsqrt(var + LN_EPS) * gain + shift).astype(BF16)
        return carry

    lax.fori_loop(0, rows // 16, norm_rows, 0)
    perm = one_hot_rows(rows, batch)
    cos_t = cos_ref[...]
    sin_t = sin_ref[...]

    def one_tile(t, carry):
        acc = jnp.dot(hid[...], w_buf[t], preferred_element_type=F32) + bias_ref[t]
        acc = acc.astype(BF16).astype(F32)
        for part in range(2):
            vals = acc[:, part * head_dim:(part + 1) * head_dim]
            cos_p, sin_p = cos_t, sin_t
            if part == 1:
                cos_p = jnp.where(t == tiles - 1, 1.0, cos_t)
                sin_p = jnp.where(t == tiles - 1, 0.0, sin_t)
            vals = vals * cos_p + pltpu.roll(vals, head_dim // 2, 1) * sin_p
            out_ref[2 * t + part] = jnp.dot(perm, vals.astype(BF16), preferred_element_type=F32)
        return carry

    def q_tile(t, carry):
        pltpu.make_async_copy(wq_any.at[:, pl.ds(pl.multiple_of(t * tile, tile), tile)], w_buf.at[t], w_sem.at[t]).wait()
        return one_tile(t, carry)

    lax.fori_loop(0, tiles - 1, q_tile, 0)
    k_copy.wait()
    v_copy.wait()
    lax.fori_loop(tiles - 1, tiles, one_tile, 0)


def attend_kernel(pos_ref, where_ref, qkv_ref, k_ref, v_ref, part_ref, kout_ref, vout_ref, *,
                  heads, steps, slots):
    batches, local, head_dim = k_ref.shape
    half = heads // 2
    first = where_ref[0]
    leader = where_ref[1]
    base_batch = pl.program_id(0) * batches
    kout_ref[...] = k_ref[...]
    vout_ref[...] = v_ref[...]
    scale = head_dim ** -0.5
    pair_rows = 2 * steps
    row = lax.broadcasted_iota(jnp.int32, (pair_rows, local), 0)
    slot = lax.broadcasted_iota(jnp.int32, (pair_rows, local), 1) + first
    step = lax.rem(row, steps)
    n_row = lax.broadcasted_iota(jnp.int32, (pair_rows, head_dim), 0)
    n_col = lax.broadcasted_iota(jnp.int32, (pair_rows, head_dim), 1)
    new_ok = ((lax.div(n_row, steps) == lax.div(n_col, steps)) & (lax.rem(n_col, steps) <= lax.rem(n_row, steps))
              & (n_col < pair_rows) & (leader == 1))
    lane = n_col
    pad = jnp.zeros((head_dim - pair_rows, head_dim), F32)
    nt = (((1,), (1,)), ((), ()))
    for pr in range(batches // 2):
        rows = slice(pair_rows * pr, pair_rows * (pr + 1))
        pos0 = pos_ref[base_batch + 2 * pr]
        pos1 = pos_ref[base_batch + 2 * pr + 1]
        cur = jnp.where(row < steps, pos0, pos1) + step
        dist = lax.rem(cur - slot + slots * (1 + (1 << 20) // slots), slots) if slots & (slots - 1) else (cur - slot) & (slots - 1)
        old_ok = ((dist > step) & (dist <= cur))[None]
        query = qkv_ref[0:heads, rows, :].reshape(heads * pair_rows, head_dim).astype(BF16)
        new_k = jnp.concatenate([qkv_ref[heads, rows, :], pad], axis=0).astype(BF16)
        new_v = jnp.concatenate([qkv_ref[heads + 1, rows, :], pad], axis=0).astype(BF16)
        score0 = lax.dot_general(query, k_ref[2 * pr], nt, preferred_element_type=F32).reshape(heads, pair_rows, local)
        score1 = lax.dot_general(query, k_ref[2 * pr + 1], nt, preferred_element_type=F32).reshape(heads, pair_rows, local)
        score = jnp.where((row < steps)[None], score0, score1) * scale
        score = jnp.where(old_ok, score, NEG_BIG)
        score_n = lax.dot_general(query, new_k, nt, preferred_element_type=F32).reshape(heads, pair_rows, head_dim) * scale
        score_n = jnp.where(new_ok[None], score_n, NEG_BIG)
        top = jnp.maximum(jnp.max(score, axis=-1, keepdims=True), jnp.max(score_n, axis=-1, keepdims=True))
        wts = jnp.where(old_ok, jnp.exp(score - top), 0.0)
        wts_n = jnp.where(new_ok[None], jnp.exp(score_n - top), 0.0)
        total = jnp.sum(wts, axis=-1, keepdims=True) + jnp.sum(wts_n, axis=-1, keepdims=True)
        wts = wts.reshape(heads * pair_rows, local).astype(BF16)
        wts_n = wts_n.reshape(heads * pair_rows, head_dim).astype(BF16)
        out0 = jnp.dot(wts, v_ref[2 * pr], preferred_element_type=F32).reshape(heads, pair_rows, head_dim)
        out1 = jnp.dot(wts, v_ref[2 * pr + 1], preferred_element_type=F32).reshape(heads, pair_rows, head_dim)
        out_n = jnp.dot(wts_n, new_v, preferred_element_type=F32).reshape(heads, pair_rows, head_dim)
        out = jnp.where((n_row < steps)[None], out0, out1) + out_n
        for core in range(2):
            part_ref[core, 0:half, rows, :] = out[core * half:(core + 1) * half]
            stat = jnp.zeros((pair_rows, head_dim), F32)
            for h in range(half):
                stat = jnp.where(lane == h, top[core * half + h], stat)
                stat = jnp.where(lane == head_dim // 2 + h, total[core * half + h], stat)
            part_ref[core, half, rows, :] = stat
    window = lax.broadcasted_iota(jnp.int32, (16, head_dim), 0)
    for b in range(batches):
        for t in range(steps):
            full = lax.rem(pos_ref[base_batch + b] + t, slots)
            at = full - first

            @pl.when((at >= 0) & (at < local))
            def _():
                start = pl.multiple_of(lax.div(at, 16) * 16, 16)
                hit = window == at - start
                for src, dst in ((heads, kout_ref), (heads + 1, vout_ref)):
                    fresh = qkv_ref[src, b * steps + t:b * steps + t + 1, :]
                    old = dst[b, pl.ds(start, 16), :].astype(F32)
                    dst[b, pl.ds(start, 16), :] = jnp.where(hit, fresh, old).astype(BF16)


def merge_parts(parts, half, head_dim):
    stats = [p[half] for p in parts]
    top = functools.reduce(jnp.maximum, stats)
    scales = [jnp.exp(s - top) for s in stats]
    lane = lax.broadcasted_iota(jnp.int32, top.shape, 1)
    total = sum(s * pltpu.roll(f, head_dim // 2, 1) for s, f in zip(stats, scales))
    stat = jnp.where(lane < head_dim // 2, top, total)
    outs = []
    for h in range(half):
        outs.append(sum(p[h] * f[:, h:h + 1] for p, f in zip(parts, scales)))
    return outs, stat


def tail_kernel(part_ref, x_any, vec_ref, bfc_ref, wo_any, wfc_any, wpj_any, y_ref,
                w_buf, x_buf, merged, pair_in, x_in, a_own, a_in, a_full, o_part, o_in, x1_all, hid, f_acc,
                g_own, g_in, p_part, p_in, y_all, w_sem, x_sem, send, recv, *, n_x, n_y, half, head_dim, col_tile):
    steps, blk_b, cols = x_buf.shape
    blk = steps * blk_b
    width = n_y * 2 * cols
    core_cols = n_y * cols
    depth = w_buf.shape[1]
    sq = lax.axis_index("sq")
    y = lax.axis_index("tp")
    x = lax.div(sq, 2)
    c = lax.rem(sq, 2)
    mine = c * n_y + y
    my_col = pl.multiple_of(mine * cols, cols)
    half_col = pl.multiple_of(c * core_cols, core_cols)

    def partner():
        return {"tp": y, "sq": 2 * x + 1 - c}

    def along_x(d):
        return {"tp": y, "sq": 2 * lax.rem(x + d, n_x) + c}

    def along_y(d):
        return {"tp": lax.rem(y + d, n_y), "sq": sq}

    ids = iter(range(1000))

    def remote(src, dst, dev):
        n = next(ids)
        return pltpu.make_async_remote_copy(src_ref=src, dst_ref=dst, send_sem=send.at[n], recv_sem=recv.at[n],
                                            device_id=dev, device_id_type=MESH)

    fc_rows = width // 4
    pj_rows = wpj_any.shape[0] // 4
    wo_copy = pltpu.make_async_copy(wo_any.at[:, pl.ds(half_col, core_cols)], w_buf.at[0], w_sem.at[0])
    fc_copy = [pltpu.make_async_copy(wfc_any.at[pl.ds(k * fc_rows, fc_rows), pl.ds(half_col, core_cols)], w_buf.at[1 + k],
                                     w_sem.at[1 + k]) for k in range(4)]
    pj_copy = []
    for k in range(4):
        side = c if k < 2 else 1 - c
        start = pl.multiple_of(side * (2 * pj_rows) + (k % 2) * pj_rows, 16)
        pj_copy.append(pltpu.make_async_copy(wpj_any.at[pl.ds(start, pj_rows), pl.ds(half_col, core_cols)], w_buf.at[k],
                                             w_sem.at[5 + k]))
    x_copy = pltpu.make_async_copy(x_any.at[:, pl.ds(pl.multiple_of(x * blk_b, blk_b), blk_b), pl.ds(my_col, cols)], x_buf, x_sem)
    x_copy.start()
    wo_copy.start()
    fc_copy[0].start()

    barrier = pltpu.get_barrier_semaphore()
    peers = [partner()] + [along_x(d) for d in range(1, n_x)] + [along_y(d) for d in range(1, n_y)]
    for dev in peers:
        pl.semaphore_signal(barrier, inc=1, device_id=dev, device_id_type=MESH)
    pl.semaphore_wait(barrier, len(peers))

    sent = []
    pair = remote(part_ref.at[1 - c], pair_in, partner())
    pair.start()
    sent.append(pair)
    pair.wait_recv()
    hops = []
    for d in list(range(1, n_x)) + [0]:
        at = pl.ds(pl.multiple_of(lax.rem(x + d, n_x) * blk, blk), blk)
        own = [part_ref[c, h, at, :] for h in range(half + 1)]
        other = [pair_in[h, at, :] for h in range(half + 1)]
        outs, stat = merge_parts([own, other], half, head_dim)
        for h in range(half):
            merged[h, at, :] = outs[h]
        merged[half, at, :] = stat
        if d:
            hop = remote(merged.at[:, at, :], x_in.at[d - 1], along_x(d))
            hop.start()
            hops.append(hop)
    fc_copy[1].start()
    fc_copy[2].start()
    for hop in hops:
        hop.wait_recv()
    sent += hops
    at = pl.ds(pl.multiple_of(x * blk, blk), blk)
    parts = [[merged[h, at, :] for h in range(half + 1)]]
    for d in range(n_x - 1):
        parts.append([x_in[d, h] for h in range(half + 1)])
    outs, stat = merge_parts(parts, half, head_dim)
    for h in range(half):
        denom = stat[:, head_dim // 2 + h:head_dim // 2 + h + 1]
        a_own[:, h * head_dim:(h + 1) * head_dim] = (outs[h] / denom).astype(BF16).astype(F32)
    a_copy = remote(a_own, a_in, partner())
    a_copy.start()
    sent.append(a_copy)
    fc_copy[3].start()
    perm = one_hot_rows(blk, steps)
    a_cols = half * head_dim
    a_full[:, pl.ds(pl.multiple_of(c * a_cols, a_cols), a_cols)] = jnp.dot(
        perm, a_own[...].astype(BF16), preferred_element_type=F32).astype(BF16)
    a_copy.wait_recv()
    a_full[:, pl.ds(pl.multiple_of((1 - c) * a_cols, a_cols), a_cols)] = jnp.dot(
        perm, a_in[...].astype(BF16), preferred_element_type=F32).astype(BF16)

    wo_copy.wait()
    order = [d for d in (2, 1, 3) if d < n_y] + [d for d in range(4, n_y)] + [0]
    hops = {}
    for d in order:
        at = pl.ds(pl.multiple_of(lax.rem(y + d, n_y) * cols, cols), cols)
        o_part[:, at] = jnp.dot(a_full[...], w_buf[0, :, at], preferred_element_type=F32)
        if d:
            hops[d] = remote(o_part.at[:, at], o_in.at[d - 1], along_y(d))
            hops[d].start()
    pj_copy[0].start()
    x_copy.wait()
    at = pl.ds(pl.multiple_of(y * cols, cols), cols)
    acc = o_part[:, at]
    for d in order[:-1]:
        hops[d].wait_recv()
        sent.append(hops[d])
        acc = acc + o_in[d - 1]
    x_mid = x_buf[...].astype(F32).reshape(blk, cols) + acc + vec_ref[2:3, pl.ds(my_col, cols)]
    x1_all[mine] = x_mid.astype(BF16).astype(F32)

    hops = [remote(x1_all.at[mine], x1_all.at[mine], along_y(d)) for d in range(1, n_y)]
    for hop in hops:
        hop.start()
    fwd = [remote(x1_all.at[mine], x1_all.at[mine], partner())]
    fwd[0].start()
    for d in range(1, n_y):
        hops[d - 1].wait_recv()
        slot = c * n_y + lax.rem(y - d + n_y, n_y)
        fwd.append(remote(x1_all.at[slot], x1_all.at[slot], partner()))
        fwd[-1].start()
    for hop in fwd:
        hop.wait_recv()
    sent += hops + fwd

    total = jnp.zeros((blk, 1), F32)
    for i in range(2 * n_y):
        total = total + jnp.sum(x1_all[i], axis=-1, keepdims=True)
    mean = total * (1.0 / width)
    total = jnp.zeros((blk, 1), F32)
    for i in range(2 * n_y):
        dev = x1_all[i] - mean
        total = total + jnp.sum(dev * dev, axis=-1, keepdims=True)
    inv = lax.rsqrt(total * (1.0 / width) + LN_EPS)
    for i in range(2 * n_y):
        at = slice(i * cols, (i + 1) * cols)
        hid[:, at] = ((x1_all[i] - mean) * inv * vec_ref[4:5, at] + vec_ref[5:6, at]).astype(BF16)

    tiles = core_cols // col_tile
    for k in range(4):
        fc_copy[k].wait()

        def fc_tile(j, carry, k=k):
            at = pl.ds(pl.multiple_of(j * col_tile, col_tile), col_tile)
            val = jnp.dot(hid[:, k * fc_rows:(k + 1) * fc_rows], w_buf[1 + k, :, at], preferred_element_type=F32)
            if k > 0:
                val = val + f_acc[:, at]
            if k < 3:
                f_acc[:, at] = val
            else:
                val = val + bfc_ref[:, pl.ds(pl.multiple_of(half_col + j * col_tile, col_tile), col_tile)]
                g_own[:, at] = jax.nn.gelu(val, approximate=True).astype(BF16).astype(F32)
            return carry

        lax.fori_loop(0, tiles, fc_tile, 0)
        if k < 3:
            pj_copy[k + 1].start()
    g_copy = remote(g_own, g_in, partner())
    g_copy.start()
    sent.append(g_copy)
    for k in range(3):
        if k == 2:
            g_copy.wait_recv()
        pj_copy[k].wait()
        left = g_own if k < 2 else g_in

        def pj_tile(j, carry, k=k, left=left):
            at = pl.ds(pl.multiple_of(j * col_tile, col_tile), col_tile)
            lhs = left[:, (k % 2) * pj_rows:(k % 2 + 1) * pj_rows].astype(BF16)
            val = jnp.dot(lhs, w_buf[k, :, at], preferred_element_type=F32)
            if k > 0:
                val = val + p_part[:, at]
            p_part[:, at] = val
            return carry

        lax.fori_loop(0, tiles, pj_tile, 0)
    pj_copy[3].wait()
    hops = {}
    for d in order:
        at = pl.ds(pl.multiple_of(lax.rem(y + d, n_y) * cols, cols), cols)
        p_part[:, at] = p_part[:, at] + jnp.dot(g_in[:, pj_rows:2 * pj_rows].astype(BF16), w_buf[3, :, at],
                                                preferred_element_type=F32)
        if d:
            hops[d] = remote(p_part.at[:, at], p_in.at[d - 1], along_y(d))
            hops[d].start()
    at = pl.ds(pl.multiple_of(y * cols, cols), cols)
    acc = p_part[:, at]
    for d in order[:-1]:
        hops[d].wait_recv()
        sent.append(hops[d])
        acc = acc + p_in[d - 1]
    y_all[x, mine] = (x1_all[mine] + acc + vec_ref[3:4, pl.ds(my_col, cols)]).astype(BF16).astype(F32)

    upper, lower = pl.ds(0, blk // 2), pl.ds(blk // 2, blk // 2)
    own_slots = pl.ds(c * n_y, n_y)
    up1, low1 = [], []
    for d in range(1, max(n_x, n_y)):
        if d < n_x:
            up1.append(remote(y_all.at[x, mine, upper], y_all.at[x, mine, upper], along_x(d)))
            up1[-1].start()
        if d < n_y:
            low1.append(remote(y_all.at[x, mine, lower], y_all.at[x, mine, lower], along_y(d)))
            low1[-1].start()
    for hop in up1:
        hop.wait_recv()
    view = y_all.at[:, mine, upper]
    up2 = [remote(view, view, along_y(d)) for d in range(1, n_y)]
    for hop in up2:
        hop.start()
    fwd = [remote(view, view, partner())]
    for hop in low1:
        hop.wait_recv()
    view = y_all.at[x, own_slots, lower]
    low2 = [remote(view, view, along_x(d)) for d in range(1, n_x)]
    for hop in low2:
        hop.start()
    fwd.append(remote(view, view, partner()))
    fwd[0].start()
    fwd[1].start()
    for d in range(1, max(n_x, n_y)):
        if d < n_y:
            up2[d - 1].wait_recv()
            view = y_all.at[:, c * n_y + lax.rem(y - d + n_y, n_y), upper]
            fwd.append(remote(view, view, partner()))
            fwd[-1].start()
        if d < n_x:
            low2[d - 1].wait_recv()
            view = y_all.at[lax.rem(x - d + n_x, n_x), own_slots, lower]
            fwd.append(remote(view, view, partner()))
            fwd[-1].start()
    for hop in fwd:
        hop.wait_recv()
    sent += up1 + low1 + up2 + low2 + fwd
    for s in range(steps):
        for xb in range(0, n_x, 2):
            for i in range(2 * n_y):
                block = jnp.concatenate([y_all[xb, i, s * blk_b:(s + 1) * blk_b, :],
                                         y_all[xb + 1, i, s * blk_b:(s + 1) * blk_b, :]], axis=0)
                y_ref[s, xb * blk_b:(xb + 2) * blk_b, i * cols:(i + 1) * cols] = block.astype(BF16)
    for hop in sent:
        hop.wait_send()


def solution(mesh):
    n_sq = mesh.shape["sq"]
    n_y = mesh.shape["tp"]
    n_x = n_sq // 2
    act_spec = P(None, "dp", None)
    cache_spec = P("dp", "sq", "tp", None)
    col_spec = P(None, "tp")
    row_spec = P("tp", None)
    vec_spec = P("tp")
    rep_spec = P(None)
    in_specs = (act_spec, P("dp"), cache_spec, cache_spec, col_spec, vec_spec, col_spec, vec_spec,
                col_spec, vec_spec, row_spec, rep_spec, rep_spec, rep_spec, rep_spec, rep_spec,
                col_spec, vec_spec, row_spec, rep_spec)
    out_specs = (act_spec, cache_spec, cache_spec)
    vmem = pl.BlockSpec(memory_space=pltpu.VMEM)
    hbm = pl.BlockSpec(memory_space=pl.ANY)

    def per_device(x_steps, positions, key_buf, val_buf, w_q, b_q, w_k, b_k, w_v, b_v, w_o, b_o,
                   ln1_gain, ln1_bias, ln2_gain, ln2_bias, w_fc, b_fc, w_proj, b_proj):
        steps, batch, width = x_steps.shape
        local, head_dim = key_buf.shape[1], key_buf.shape[3]
        slots = local * n_sq
        rows = steps * batch
        heads = w_q.shape[1] // head_dim
        half = heads // 2
        tile = 2 * head_dim
        tiles = w_q.shape[1] // tile + 1
        vecs = jnp.stack([ln1_gain, ln1_bias, b_o, b_proj, ln2_gain, ln2_bias]).astype(F32)
        qkv_bias = jnp.concatenate([b_q, b_k, b_v]).astype(F32).reshape(tiles, 1, tile)
        half_dim = head_dim // 2
        inv_freq = jnp.power(jnp.float32(ROPE_BASE), -2.0 * jnp.arange(half_dim, dtype=F32) / head_dim)
        cur = positions[None, :] + jnp.arange(steps, dtype=jnp.int32)[:, None]
        angle = cur.reshape(rows).astype(F32)[:, None] * inv_freq
        cos_t, sin_t = jnp.cos(angle), jnp.sin(angle)
        cos_t = jnp.concatenate([cos_t, cos_t], axis=-1)
        sin_t = jnp.concatenate([-sin_t, sin_t], axis=-1)

        qkv = pl.pallas_call(
            functools.partial(qkv_kernel, batch=batch, tiles=tiles, tile=tile, head_dim=head_dim),
            out_shape=jax.ShapeDtypeStruct((heads + 2, rows, head_dim), F32),
            in_specs=[hbm, hbm, hbm, hbm, vmem, vmem, vmem, vmem],
            out_specs=vmem,
            scratch_shapes=[pltpu.VMEM((rows, width), BF16), pltpu.VMEM((tiles, width, tile), BF16),
                            pltpu.VMEM((rows, width), BF16), pltpu.SemaphoreType.DMA,
                            pltpu.SemaphoreType.DMA((tiles + 1,))],
            compiler_params=pltpu.CompilerParams(vmem_limit_bytes=VMEM_BYTES),
            name="qkv",
        )(x_steps.reshape(rows, width), w_q, w_k, w_v, qkv_bias, vecs, cos_t, sin_t)

        sq = lax.axis_index("sq")
        place = jnp.stack([sq * local, jnp.where(sq == 0, 1, 0)]).astype(jnp.int32)
        per = 4
        kv_spec = pl.BlockSpec((per, local, head_dim), lambda i, *_: (i, 0, 0))
        part, k_new, v_new = pl.pallas_call(
            functools.partial(attend_kernel, heads=heads, steps=steps, slots=slots),
            out_shape=(jax.ShapeDtypeStruct((2, half + 1, rows, head_dim), F32),
                       jax.ShapeDtypeStruct((batch, local, head_dim), BF16),
                       jax.ShapeDtypeStruct((batch, local, head_dim), BF16)),
            grid_spec=pltpu.PrefetchScalarGridSpec(
                num_scalar_prefetch=2, grid=(batch // per,),
                in_specs=[pl.BlockSpec((heads + 2, per * steps, head_dim), lambda i, *_: (0, i, 0)), kv_spec, kv_spec],
                out_specs=(pl.BlockSpec((2, half + 1, per * steps, head_dim), lambda i, *_: (0, 0, i, 0)), kv_spec, kv_spec)),
            compiler_params=pltpu.CompilerParams(dimension_semantics=("arbitrary",), vmem_limit_bytes=VMEM_BYTES),
            name="attend",
        )(positions, place, qkv, key_buf.reshape(batch, local, head_dim), val_buf.reshape(batch, local, head_dim))

        cols = width // (2 * n_y)
        core_cols = width // 2
        blk_b = batch // n_x
        blk = blk_b * steps
        depth = w_o.shape[0]
        ys = pl.pallas_call(
            functools.partial(tail_kernel, n_x=n_x, n_y=n_y, half=half, head_dim=head_dim, col_tile=min(512, core_cols)),
            out_shape=jax.ShapeDtypeStruct((steps, batch, width), BF16),
            in_specs=[vmem, hbm, vmem, vmem, hbm, hbm, hbm],
            out_specs=vmem,
            scratch_shapes=[
                pltpu.VMEM((5, depth, core_cols), BF16),
                pltpu.VMEM((steps, blk_b, cols), BF16),
                pltpu.VMEM((half + 1, rows, head_dim), F32),
                pltpu.VMEM((half + 1, rows, head_dim), F32),
                pltpu.VMEM((n_x - 1, half + 1, blk, head_dim), F32),
                pltpu.VMEM((blk, half * head_dim), F32),
                pltpu.VMEM((blk, half * head_dim), F32),
                pltpu.VMEM((blk, heads * head_dim), BF16),
                pltpu.VMEM((blk, core_cols), F32),
                pltpu.VMEM((n_y - 1, blk, cols), F32),
                pltpu.VMEM((2 * n_y, blk, cols), F32),
                pltpu.VMEM((blk, width), BF16),
                pltpu.VMEM((blk, core_cols), F32),
                pltpu.VMEM((blk, core_cols), F32),
                pltpu.VMEM((blk, core_cols), F32),
                pltpu.VMEM((blk, core_cols), F32),
                pltpu.VMEM((n_y - 1, blk, cols), F32),
                pltpu.VMEM((n_x, 2 * n_y, blk, cols), F32),
                pltpu.SemaphoreType.DMA((9,)),
                pltpu.SemaphoreType.DMA,
                pltpu.SemaphoreType.DMA((48,)),
                pltpu.SemaphoreType.DMA((48,)),
            ],
            compiler_params=pltpu.CompilerParams(collective_id=0, has_side_effects=True, vmem_limit_bytes=VMEM_BYTES),
            name="tail",
        )(part, x_steps, vecs, b_fc.astype(F32).reshape(1, -1), w_o, w_fc, w_proj)
        return ys, k_new.reshape(key_buf.shape), v_new.reshape(val_buf.shape)

    return jax.shard_map(per_device, mesh=mesh, in_specs=in_specs, out_specs=out_specs, check_vma=False)
```

```python
import functools

import jax
import jax.numpy as jnp
from jax import lax
from jax.experimental import pallas as pl
from jax.experimental.pallas import tpu as pltpu
from jax.sharding import PartitionSpec as P

ROPE_BASE = 1000000.0
LN_EPS = 1e-5
NEG_BIG = -1e30
MESH = pl.DeviceIdType.MESH
F32 = jnp.float32
BF16 = jnp.bfloat16
VMEM_BYTES = 67043328


def one_hot_rows(size, inner):
    outer = size // inner
    row = lax.broadcasted_iota(jnp.int32, (size, size), 0)
    col = lax.broadcasted_iota(jnp.int32, (size, size), 1)
    source = lax.rem(row, outer) * inner + lax.div(row, outer)
    return jnp.where(col == source, 1.0, 0.0).astype(BF16)


def front_kernel(pos_ref, x_any, wq_any, wk_any, wv_any, vec_ref, cos_ref, sin_ref, kc_any, vc_any,
                 part_ref, kout_any, vout_any,
                 x_buf, hid, wq_buf, wk_buf, wv_buf, acc, qkv, k_buf, v_buf,
                 x_sem, wq_sem, kv_sem, c_sem, out_sem, *, batch, heads, head_dim, steps, per):
    rows, width = x_buf.shape
    n_q = heads * head_dim
    bands, band = wq_buf.shape[0], wq_buf.shape[1]
    local = k_buf.shape[1]
    slots = local * lax.axis_size("sq")
    groups = batch // per
    half = heads // 2
    first = lax.axis_index("sq") * local
    leader = lax.axis_index("sq") == 0

    x_copy = pltpu.make_async_copy(x_any, x_buf, x_sem)
    x_copy.start()
    k_copy = pltpu.make_async_copy(wk_any, wk_buf, kv_sem.at[0])
    v_copy = pltpu.make_async_copy(wv_any, wv_buf, kv_sem.at[1])
    k_copy.start()
    v_copy.start()

    def q_copy(i):
        return pltpu.make_async_copy(wq_any.at[pl.ds(pl.multiple_of(i * band, band), band), :], wq_buf.at[i], wq_sem.at[i])

    def cache_in(i):
        at = pl.ds(i * per, per)
        return (pltpu.make_async_copy(kc_any.at[at], k_buf.at[at], c_sem.at[0, i]),
                pltpu.make_async_copy(vc_any.at[at], v_buf.at[at], c_sem.at[1, i]))

    def cache_out(i):
        at = pl.ds(i * per, per)
        return (pltpu.make_async_copy(k_buf.at[at], kout_any.at[at], out_sem.at[0, i]),
                pltpu.make_async_copy(v_buf.at[at], vout_any.at[at], out_sem.at[1, i]))

    for i in range(bands):
        q_copy(i).start()
    for i in range(groups):
        for cp in cache_in(i):
            cp.start()

    gain = vec_ref[0:1, 0:width]
    shift = vec_ref[0:1, width:2 * width]
    x_copy.wait()

    def norm_rows(i, carry):
        at = pl.ds(pl.multiple_of(i * 16, 16), 16)
        vals = x_buf[at, :].astype(F32)
        mean = jnp.sum(vals, axis=-1, keepdims=True) * (1.0 / width)
        vals = vals - mean
        var = jnp.sum(vals * vals, axis=-1, keepdims=True) * (1.0 / width)
        hid[at, :] = (vals * lax.rsqrt(var + LN_EPS) * gain + shift).astype(BF16)
        return carry

    lax.fori_loop(0, rows // 16, norm_rows, 0)

    bias0 = vec_ref.shape[1] - n_q - 2 * head_dim
    perm = one_hot_rows(rows, batch)
    cos_t = cos_ref[...]
    sin_t = sin_ref[...]

    def rotate(vals):
        return vals * cos_t + pltpu.roll(vals, head_dim // 2, 1) * sin_t

    def by_batch(vals):
        return jnp.dot(perm, vals.astype(BF16), preferred_element_type=F32)

    k_copy.wait()
    v_copy.wait()
    k_new = jnp.dot(hid[...], wk_buf[...], preferred_element_type=F32) + vec_ref[0:1, bias0 + n_q:bias0 + n_q + head_dim]
    v_new = jnp.dot(hid[...], wv_buf[...], preferred_element_type=F32) + vec_ref[0:1, bias0 + n_q + head_dim:]
    qkv[heads] = by_batch(rotate(k_new.astype(BF16).astype(F32)))
    qkv[heads + 1] = by_batch(v_new)
    acc[...] = jnp.broadcast_to(vec_ref[0:1, bias0:bias0 + n_q], acc.shape)

    def q_band(i, carry):
        q_copy(i).wait()
        acc[...] += jnp.dot(hid[:, pl.ds(pl.multiple_of(i * band, band), band)], wq_buf[i], preferred_element_type=F32)
        return carry

    lax.fori_loop(0, bands, q_band, 0)

    def q_head(h, carry):
        vals = acc[:, pl.ds(pl.multiple_of(h * head_dim, head_dim), head_dim)]
        qkv[h] = by_batch(rotate(vals.astype(BF16).astype(F32)))
        return carry

    lax.fori_loop(0, heads, q_head, 0)

    scale = head_dim ** -0.5
    pair_rows = 2 * steps
    row = lax.broadcasted_iota(jnp.int32, (pair_rows, local), 0)
    slot = lax.broadcasted_iota(jnp.int32, (pair_rows, local), 1) + first
    step = lax.rem(row, steps)
    n_row = lax.broadcasted_iota(jnp.int32, (pair_rows, head_dim), 0)
    n_col = lax.broadcasted_iota(jnp.int32, (pair_rows, head_dim), 1)
    new_ok = ((lax.div(n_row, steps) == lax.div(n_col, steps)) & (lax.rem(n_col, steps) <= lax.rem(n_row, steps))
              & (n_col < pair_rows) & leader)[None]
    lane = n_col
    pad = jnp.zeros((head_dim - pair_rows, head_dim), F32)
    window = lax.broadcasted_iota(jnp.int32, (16, head_dim), 0)
    nt = (((1,), (1,)), ((), ()))

    def group(i, carry):
        for cp in cache_in(i):
            cp.wait()
        for pr in range(per // 2):
            b0 = i * per + 2 * pr
            rows_at = pl.ds(pl.multiple_of(i * (per * steps) + pair_rows * pr, pair_rows), pair_rows)
            pos0 = pos_ref[b0]
            pos1 = pos_ref[b0 + 1]
            cur = jnp.where(row < steps, pos0, pos1) + step
            if slots & (slots - 1):
                dist = lax.rem(lax.rem(cur - slot, slots) + slots, slots)
            else:
                dist = (cur - slot) & (slots - 1)
            old_ok = ((dist > step) & (dist <= cur))[None]
            query = qkv[0:heads, rows_at, :].reshape(heads * pair_rows, head_dim).astype(BF16)
            new_k = jnp.concatenate([qkv[heads, rows_at, :], pad], axis=0).astype(BF16)
            new_v = jnp.concatenate([qkv[heads + 1, rows_at, :], pad], axis=0).astype(BF16)
            shape = (heads, pair_rows, local)
            score0 = lax.dot_general(query, k_buf[b0], nt, preferred_element_type=F32).reshape(shape)
            score1 = lax.dot_general(query, k_buf[b0 + 1], nt, preferred_element_type=F32).reshape(shape)
            score = jnp.where(old_ok, jnp.where((row < steps)[None], score0, score1) * scale, NEG_BIG)
            shape = (heads, pair_rows, head_dim)
            score_n = lax.dot_general(query, new_k, nt, preferred_element_type=F32).reshape(shape) * scale
            score_n = jnp.where(new_ok, score_n, NEG_BIG)
            top = jnp.max(jnp.maximum(score_n, functools.reduce(
                jnp.maximum, [score[:, :, j:j + head_dim] for j in range(0, local, head_dim)])), axis=-1, keepdims=True)
            wts = jnp.where(old_ok, jnp.exp(score - top), 0.0)
            wts_n = jnp.where(new_ok, jnp.exp(score_n - top), 0.0)
            total = jnp.sum(wts_n + sum(wts[:, :, j:j + head_dim] for j in range(0, local, head_dim)), axis=-1, keepdims=True)
            wts = wts.reshape(heads * pair_rows, local).astype(BF16)
            wts_n = wts_n.reshape(heads * pair_rows, head_dim).astype(BF16)
            out0 = jnp.dot(wts, v_buf[b0], preferred_element_type=F32).reshape(shape)
            out1 = jnp.dot(wts, v_buf[b0 + 1], preferred_element_type=F32).reshape(shape)
            out_n = jnp.dot(wts_n, new_v, preferred_element_type=F32).reshape(shape)
            out = jnp.where((n_row < steps)[None], out0, out1) + out_n
            for core in range(2):
                part_ref[core, 0:half, rows_at, :] = out[core * half:(core + 1) * half]
                stat = jnp.zeros((pair_rows, head_dim), F32)
                for h in range(half):
                    stat = jnp.where(lane == h, top[core * half + h], stat)
                    stat = jnp.where(lane == head_dim // 2 + h, total[core * half + h], stat)
                part_ref[core, half, rows_at, :] = stat
        for b in range(per):
            for t in range(steps):
                at = lax.rem(pos_ref[i * per + b] + t, slots) - first

                @pl.when((at >= 0) & (at < local))
                def _(b=b, t=t, at=at):
                    start = pl.multiple_of(lax.div(at, 16) * 16, 16)
                    hit = window == at - start
                    for src, dst in ((heads, k_buf), (heads + 1, v_buf)):
                        fresh = qkv[src, pl.ds(i * (per * steps) + b * steps + t, 1), :]
                        old = dst[i * per + b, pl.ds(start, 16), :].astype(F32)
                        dst[i * per + b, pl.ds(start, 16), :] = jnp.where(hit, fresh, old).astype(BF16)

        for cp in cache_out(i):
            cp.start()
        return carry

    lax.fori_loop(0, groups, group, 0)
    for i in range(groups):
        for cp in cache_out(i):
            cp.wait()


def merge_parts(parts, half, head_dim):
    stats = [p[half] for p in parts]
    top = functools.reduce(jnp.maximum, stats)
    scales = [jnp.exp(s - top) for s in stats]
    lane = lax.broadcasted_iota(jnp.int32, top.shape, 1)
    total = sum(s * pltpu.roll(f, head_dim // 2, 1) for s, f in zip(stats, scales))
    stat = jnp.where(lane < head_dim // 2, top, total)
    outs = []
    for h in range(half):
        outs.append(sum(p[h] * f[:, h:h + 1] for p, f in zip(parts, scales)))
    return outs, stat


def tail_kernel(part_ref, x_any, vec_ref, wo_any, wfc_any, wpj_any, y_ref,
                w_buf, x_buf, pair_in, m_part, x_in, a_own, a_in, a_full, o_part, o_in, x1_all, hid,
                g_own, g_in, g_full, p_part, p_in, y_all, w_sem, x_sem, send, recv, *, half, head_dim):
    steps, blk_b, cols = x_buf.shape
    blk = steps * blk_b
    n = 4
    width = 2 * n * cols
    core_cols = n * cols
    depth = wo_any.shape[0]
    ff = wpj_any.shape[0]
    sq = lax.axis_index("sq")
    y = lax.axis_index("tp")
    x = lax.div(sq, 2)
    c = lax.rem(sq, 2)
    mine = c * n + y
    my_col = pl.multiple_of(mine * cols, cols)
    half_col = pl.multiple_of(c * core_cols, core_cols)
    lo, hi = pl.ds(0, blk // 2), pl.ds(blk // 2, blk // 2)
    left, right = pl.ds(0, cols // 2), pl.ds(cols // 2, cols // 2)
    every = pl.ds(0, blk)
    all_cols = pl.ds(0, cols)
    partner = {"tp": y, "sq": 2 * x + 1 - c}

    def along_x(d):
        return {"tp": y, "sq": 2 * lax.rem(x + d, n) + c}

    def along_y(d):
        return {"tp": lax.rem(y + d, n), "sq": sq}

    ids = iter(range(1000))
    sent = []

    def push(src, dst, dev):
        i = next(ids)
        cp = pltpu.make_async_remote_copy(src_ref=src, dst_ref=dst, send_sem=send.at[i], recv_sem=recv.at[i],
                                          device_id=dev, device_id_type=MESH)
        cp.start()
        sent.append(cp)
        return cp

    order = (2, 1, 3, 0)

    def block_col(d):
        return pl.multiple_of(half_col + lax.rem(y + d, n) * cols, cols)

    wo_copy = [pltpu.make_async_copy(wo_any.at[:, pl.ds(block_col(d), cols)], w_buf.at[0, pl.ds(d * depth, depth)], w_sem.at[d])
               for d in range(n)]
    fc_copy = [pltpu.make_async_copy(wfc_any.at[:, pl.ds(pl.multiple_of(half_col + j * cols, cols), cols)], w_buf.at[1 + j],
                                     w_sem.at[n + j]) for j in range(n)]
    pj_copy = [pltpu.make_async_copy(wpj_any.at[:, pl.ds(block_col(d), cols)], w_buf.at[k], w_sem.at[2 * n + k])
               for k, d in enumerate(order)]
    x_copy = pltpu.make_async_copy(x_any.at[:, pl.ds(pl.multiple_of(x * blk_b, blk_b), blk_b), pl.ds(my_col, cols)], x_buf, x_sem)
    x_copy.start()
    for d in order:
        wo_copy[d].start()
    fc_copy[0].start()

    barrier = pltpu.get_barrier_semaphore()
    peers = [partner] + [along_x(d) for d in (1, 3)] + [along_y(d) for d in (1, 3)]
    for dev in peers:
        pl.semaphore_signal(barrier, inc=1, device_id=dev, device_id_type=MESH)
    pl.semaphore_wait(barrier, len(peers))

    def ring_reduce(ready, half_of, inbox, along, fold):
        ready(2)
        rel_a = push(half_of(2, lo), inbox.at[0], along(1))
        rel_b = push(half_of(2, hi), inbox.at[1], along(3))
        ready(1)
        dir_b = push(half_of(1, hi), inbox.at[2], along(1))
        ready(3)
        dir_a = push(half_of(3, lo), inbox.at[3], along(3))
        rel_a.wait_recv()
        fold(1, lo, 0)
        sum_a = push(half_of(1, lo), inbox.at[4], along(1))
        rel_b.wait_recv()
        fold(3, hi, 1)
        sum_b = push(half_of(3, hi), inbox.at[5], along(3))
        ready(0)
        for cp in (dir_b, dir_a, sum_a, sum_b):
            cp.wait_recv()

    planes = range(half + 1)
    pairs = {}
    for d in order:
        at = pl.ds(pl.multiple_of(lax.rem(x + d, n) * blk, blk), blk)
        pairs[d] = push(part_ref.at[1 - c, :, at, :], pair_in.at[d], partner)
    fc_copy[1].start()

    def pair_merge(d):
        pairs[d].wait_recv()
        at = pl.ds(pl.multiple_of(lax.rem(x + d, n) * blk, blk), blk)
        outs, stat = merge_parts([[part_ref[c, h, at, :] for h in planes], [pair_in[d, h] for h in planes]], half, head_dim)
        for h in range(half):
            m_part[d, h] = outs[h]
        m_part[d, half] = stat

    def fold_parts(d, rows, i):
        outs, stat = merge_parts([[m_part[d, h, rows, :] for h in planes], [x_in[i, h] for h in planes]], half, head_dim)
        for h in range(half):
            m_part[d, h, rows, :] = outs[h]
        m_part[d, half, rows, :] = stat

    ring_reduce(pair_merge, lambda d, rows: m_part.at[d, :, rows], x_in, along_x, fold_parts)
    for rows, terms in ((lo, (3, 4)), (hi, (2, 5))):
        parts = [[m_part[0, h, rows, :] for h in planes]] + [[x_in[i, h] for h in planes] for i in terms]
        outs, stat = merge_parts(parts, half, head_dim)
        for h in range(half):
            denom = stat[:, head_dim // 2 + h:head_dim // 2 + h + 1]
            a_own[rows, h * head_dim:(h + 1) * head_dim] = (outs[h] / denom).astype(BF16).astype(F32)
    a_copy = push(a_own, a_in, partner)
    fc_copy[2].start()
    fc_copy[3].start()
    perm = one_hot_rows(blk, steps)
    a_cols = half * head_dim
    a_full[:, pl.ds(pl.multiple_of(c * a_cols, a_cols), a_cols)] = jnp.dot(
        perm, a_own[...].astype(BF16), preferred_element_type=F32).astype(BF16)
    a_copy.wait_recv()
    a_full[:, pl.ds(pl.multiple_of((1 - c) * a_cols, a_cols), a_cols)] = jnp.dot(
        perm, a_in[...].astype(BF16), preferred_element_type=F32).astype(BF16)

    def o_block(d):
        wo_copy[d].wait()
        o_part[d] = jnp.dot(a_full[...], w_buf[0, d * depth:(d + 1) * depth, :], preferred_element_type=F32)

    def fold_o(d, rows, i):
        o_part[d, rows, :] = o_part[d, rows, :] + o_in[i]

    ring_reduce(o_block, lambda d, rows: o_part.at[d, rows], o_in, along_y, fold_o)
    pj_copy[0].start()
    x_copy.wait()
    x_own = x_buf[...].astype(F32).reshape(blk, cols) + vec_ref[0:1, pl.ds(2 * width + my_col, cols)]
    hb = blk // 2
    x1_all[mine, lo] = (x_own[:hb] + (o_part[0, lo] + (o_in[3] + o_in[4]))).astype(BF16).astype(F32)
    x1_all[mine, hi] = (x_own[hb:] + (o_part[0, hi] + (o_in[2] + o_in[5]))).astype(BF16).astype(F32)

    def x1_push(d, rows, dev):
        ref = x1_all.at[c * n + lax.rem(y + d, n), rows]
        return push(ref, ref, dev)

    p_lo = x1_push(0, lo, along_y(1))
    m_hi = x1_push(0, hi, along_y(3))
    p_hi = x1_push(0, hi, along_y(1))
    m_lo = x1_push(0, lo, along_y(3))
    fwd = [x1_push(0, every, partner)]
    p_lo.wait_recv()
    r_lo = x1_push(3, lo, along_y(1))
    m_hi.wait_recv()
    r_hi = x1_push(1, hi, along_y(3))
    p_hi.wait_recv()
    fwd.append(x1_push(3, every, partner))
    m_lo.wait_recv()
    fwd.append(x1_push(1, every, partner))
    r_lo.wait_recv()
    r_hi.wait_recv()
    fwd.append(x1_push(2, every, partner))
    for cp in fwd:
        cp.wait_recv()

    total = jnp.zeros((blk, 1), F32)
    for i in range(2 * n):
        total = total + jnp.sum(x1_all[i], axis=-1, keepdims=True)
    mean = total * (1.0 / width)
    total = jnp.zeros((blk, 1), F32)
    for i in range(2 * n):
        dev = x1_all[i] - mean
        total = total + jnp.sum(dev * dev, axis=-1, keepdims=True)
    inv = lax.rsqrt(total * (1.0 / width) + LN_EPS)
    for i in range(2 * n):
        at = slice(i * cols, (i + 1) * cols)
        gain = vec_ref[0:1, 4 * width + i * cols:4 * width + (i + 1) * cols]
        shift = vec_ref[0:1, 5 * width + i * cols:5 * width + (i + 1) * cols]
        hid[:, at] = ((x1_all[i] - mean) * inv * gain + shift).astype(BF16)

    tile = 256
    own_ff = pl.multiple_of(c * (ff // 2), ff // 2)
    g_copy = []
    for j in range(n):
        fc_copy[j].wait()

        def fc_tile(t, carry, j=j):
            at = pl.ds(pl.multiple_of(t * tile, tile), tile)
            val = jnp.dot(hid[...], w_buf[1 + j, :, at], preferred_element_type=F32)
            bias_at = pl.multiple_of(6 * width + own_ff + j * cols + t * tile, tile)
            val = val + vec_ref[0:1, pl.ds(bias_at, tile)]
            val = jax.nn.gelu(val, approximate=True).astype(BF16)
            g_own[j, :, at] = val.astype(F32)
            g_full[:, pl.ds(pl.multiple_of(own_ff + j * cols + t * tile, tile), tile)] = val
            return carry

        lax.fori_loop(0, cols // tile, fc_tile, 0)
        g_copy.append(push(g_own.at[j], g_in.at[j], partner))
        if j < n - 1:
            pj_copy[j + 1].start()
    other_ff = pl.multiple_of((1 - c) * (ff // 2), ff // 2)
    for j in range(n):
        g_copy[j].wait_recv()
        g_full[:, pl.ds(pl.multiple_of(other_ff + j * cols, cols), cols)] = g_in[j].astype(BF16)

    def p_block(d):
        k = order.index(d)
        pj_copy[k].wait()

        def pj_tile(t, carry):
            at = pl.ds(pl.multiple_of(t * tile, tile), tile)
            p_part[d, :, at] = jnp.dot(g_full[...], w_buf[k, :, at], preferred_element_type=F32)
            return carry

        lax.fori_loop(0, cols // tile, pj_tile, 0)

    def fold_p(d, rows, i):
        p_part[d, rows, :] = p_part[d, rows, :] + p_in[i]

    ring_reduce(p_block, lambda d, rows: p_part.at[d, rows], p_in, along_y, fold_p)
    bias = vec_ref[0:1, pl.ds(3 * width + my_col, cols)]
    y_all[x, mine, lo] = (x1_all[mine, lo] + (p_part[0, lo] + (p_in[3] + p_in[4])) + bias).astype(BF16).astype(F32)
    y_all[x, mine, hi] = (x1_all[mine, hi] + (p_part[0, hi] + (p_in[2] + p_in[5])) + bias).astype(BF16).astype(F32)

    def unit(dx, dy, rows=every, at=all_cols):
        return y_all.at[lax.rem(x + dx, n), c * n + lax.rem(y + dy, n), rows, at]

    def relay(dx, dy, dev, rows=every, at=all_cols):
        ref = unit(dx, dy, rows, at)
        return push(ref, ref, dev)

    fwd = []

    def forward(dx, dy):
        fwd.append(relay(dx, dy, partner))

    xp, xm, yp, ym = along_x(1), along_x(3), along_y(1), along_y(3)
    o_xp, o_xm, o_yp, o_ym = [relay(0, 0, dev) for dev in (xp, xm, yp, ym)]
    forward(0, 0)
    o_xp.wait_recv()
    r_xp = relay(3, 0, xp, at=left)
    a_yp, a_ym = relay(3, 0, yp, rows=lo), relay(3, 0, ym, rows=lo)
    o_xm.wait_recv()
    r_xm = relay(1, 0, xm, at=right)
    b_yp, b_ym = relay(1, 0, yp, rows=lo), relay(1, 0, ym, rows=lo)
    o_yp.wait_recv()
    r_yp = relay(0, 3, yp, at=left)
    a_xp, a_xm = relay(0, 3, xp, rows=hi), relay(0, 3, xm, rows=hi)
    o_ym.wait_recv()
    r_ym = relay(0, 1, ym, at=right)
    b_xp, b_xm = relay(0, 1, xp, rows=hi), relay(0, 1, xm, rows=hi)
    for d in ((3, 0), (1, 0), (0, 3), (0, 1)):
        forward(*d)
    r_xp.wait_recv()
    c_yp, c_ym = relay(2, 0, yp, lo, left), relay(2, 0, ym, lo, left)
    r_xm.wait_recv()
    d_yp, d_ym = relay(2, 0, yp, lo, right), relay(2, 0, ym, lo, right)
    r_yp.wait_recv()
    c_xp, c_xm = relay(0, 2, xp, hi, left), relay(0, 2, xm, hi, left)
    r_ym.wait_recv()
    d_xp, d_xm = relay(0, 2, xp, hi, right), relay(0, 2, xm, hi, right)
    forward(2, 0)
    forward(0, 2)
    late = []
    for cp, dx, dy, dev, rows, at in ((a_yp, 3, 3, yp, lo, left), (a_ym, 3, 1, ym, lo, right),
                                      (b_yp, 1, 3, yp, lo, left), (b_ym, 1, 1, ym, lo, right),
                                      (a_xp, 3, 3, xp, hi, left), (a_xm, 1, 3, xm, hi, right),
                                      (b_xp, 3, 1, xp, hi, left), (b_xm, 1, 1, xm, hi, right)):
        cp.wait_recv()
        late.append(relay(dx, dy, dev, rows, at))
    for d in ((3, 3), (3, 1), (1, 3), (1, 1)):
        forward(*d)
    for cp, dx, dy, dev, rows, at in ((c_yp, 2, 3, yp, lo, left), (d_ym, 2, 1, ym, lo, right),
                                      (c_xp, 3, 2, xp, hi, left), (d_xm, 1, 2, xm, hi, right)):
        cp.wait_recv()
        late.append(relay(dx, dy, dev, rows, at))
    for cp in (c_ym, d_yp, c_xm, d_xp):
        cp.wait_recv()
    for cp in late[:8]:
        cp.wait_recv()
    for d in ((3, 2), (1, 2), (2, 3), (2, 1)):
        forward(*d)
    for cp in late[8:]:
        cp.wait_recv()
    forward(2, 2)
    for cp in fwd:
        cp.wait_recv()
    for s in range(steps):
        for xb in range(0, n, 2):
            for i in range(2 * n):
                block = jnp.concatenate([y_all[xb, i, s * blk_b:(s + 1) * blk_b, :],
                                         y_all[xb + 1, i, s * blk_b:(s + 1) * blk_b, :]], axis=0)
                y_ref[s, xb * blk_b:(xb + 2) * blk_b, i * cols:(i + 1) * cols] = block.astype(BF16)
    for cp in sent:
        cp.wait_send()


def solution(mesh):
    n_sq = mesh.shape["sq"]
    n_y = mesh.shape["tp"]
    n_x = n_sq // 2
    act_spec = P(None, "dp", None)
    cache_spec = P("dp", "sq", "tp", None)
    col_spec = P(None, "tp")
    row_spec = P("tp", None)
    vec_spec = P("tp")
    rep_spec = P(None)
    in_specs = (act_spec, P("dp"), cache_spec, cache_spec, col_spec, vec_spec, col_spec, vec_spec,
                col_spec, vec_spec, row_spec, rep_spec, rep_spec, rep_spec, rep_spec, rep_spec,
                col_spec, vec_spec, row_spec, rep_spec)
    out_specs = (act_spec, cache_spec, cache_spec)
    vmem = pl.BlockSpec(memory_space=pltpu.VMEM)
    hbm = pl.BlockSpec(memory_space=pl.ANY)

    def per_device(x_steps, positions, key_buf, val_buf, w_q, b_q, w_k, b_k, w_v, b_v, w_o, b_o,
                   ln1_gain, ln1_bias, ln2_gain, ln2_bias, w_fc, b_fc, w_proj, b_proj):
        steps, batch, width = x_steps.shape
        local, head_dim = key_buf.shape[1], key_buf.shape[3]
        rows = steps * batch
        heads = w_q.shape[1] // head_dim
        half = heads // 2
        vecs = jnp.concatenate([v.astype(F32) for v in (ln1_gain, ln1_bias, b_o, b_proj, ln2_gain, ln2_bias,
                                                        b_fc, b_q, b_k, b_v)]).reshape(1, -1)
        half_dim = head_dim // 2
        inv_freq = jnp.power(jnp.float32(ROPE_BASE), -2.0 * jnp.arange(half_dim, dtype=F32) / head_dim)
        inv_freq = jnp.concatenate([inv_freq, inv_freq])[None, None, :]
        sign = jnp.where(jnp.arange(head_dim) < half_dim, -1.0, 1.0).astype(F32)
        cur = positions[None, :, None] + jnp.arange(steps, dtype=jnp.int32)[:, None, None]
        angle = cur.astype(F32) * inv_freq
        cos_t = jnp.cos(angle).reshape(rows, head_dim)
        sin_t = (jnp.sin(angle) * sign).reshape(rows, head_dim)

        per, bands = 4, 6
        groups = batch // per
        smem = pl.BlockSpec(memory_space=pltpu.SMEM)
        part, k_new, v_new = pl.pallas_call(
            functools.partial(front_kernel, batch=batch, heads=heads, head_dim=head_dim, steps=steps, per=per),
            out_shape=(jax.ShapeDtypeStruct((2, half + 1, rows, head_dim), F32),
                       jax.ShapeDtypeStruct((batch, local, head_dim), BF16),
                       jax.ShapeDtypeStruct((batch, local, head_dim), BF16)),
            in_specs=[smem, hbm, hbm, hbm, hbm, vmem, vmem, vmem, hbm, hbm],
            out_specs=(vmem, hbm, hbm),
            scratch_shapes=[
                pltpu.VMEM((rows, width), BF16),
                pltpu.VMEM((rows, width), BF16),
                pltpu.VMEM((bands, width // bands, heads * head_dim), BF16),
                pltpu.VMEM((width, head_dim), BF16),
                pltpu.VMEM((width, head_dim), BF16),
                pltpu.VMEM((rows, heads * head_dim), F32),
                pltpu.VMEM((heads + 2, rows, head_dim), F32),
                pltpu.VMEM((batch, local, head_dim), BF16),
                pltpu.VMEM((batch, local, head_dim), BF16),
                pltpu.SemaphoreType.DMA,
                pltpu.SemaphoreType.DMA((bands,)),
                pltpu.SemaphoreType.DMA((2,)),
                pltpu.SemaphoreType.DMA((2, groups)),
                pltpu.SemaphoreType.DMA((2, groups)),
            ],
            compiler_params=pltpu.CompilerParams(vmem_limit_bytes=VMEM_BYTES),
            name="front",
        )(positions, x_steps.reshape(rows, width), w_q, w_k, w_v, vecs, cos_t, sin_t,
          key_buf.reshape(batch, local, head_dim), val_buf.reshape(batch, local, head_dim))

        cols = width // (2 * n_y)
        core_cols = width // 2
        blk_b = batch // n_x
        blk = blk_b * steps
        ys = pl.pallas_call(
            functools.partial(tail_kernel, half=half, head_dim=head_dim),
            out_shape=jax.ShapeDtypeStruct((steps, batch, width), BF16),
            in_specs=[vmem, hbm, vmem, hbm, hbm, hbm],
            out_specs=vmem,
            scratch_shapes=[
                pltpu.VMEM((5, width, cols), BF16),
                pltpu.VMEM((steps, blk_b, cols), BF16),
                pltpu.VMEM((4, half + 1, blk, head_dim), F32),
                pltpu.VMEM((4, half + 1, blk, head_dim), F32),
                pltpu.VMEM((6, half + 1, blk // 2, head_dim), F32),
                pltpu.VMEM((blk, half * head_dim), F32),
                pltpu.VMEM((blk, half * head_dim), F32),
                pltpu.VMEM((blk, heads * head_dim), BF16),
                pltpu.VMEM((4, blk, cols), F32),
                pltpu.VMEM((6, blk // 2, cols), F32),
                pltpu.VMEM((8, blk, cols), F32),
                pltpu.VMEM((blk, width), BF16),
                pltpu.VMEM((4, blk, cols), F32),
                pltpu.VMEM((4, blk, cols), F32),
                pltpu.VMEM((blk, w_proj.shape[0]), BF16),
                pltpu.VMEM((4, blk, cols), F32),
                pltpu.VMEM((6, blk // 2, cols), F32),
                pltpu.VMEM((4, 8, blk, cols), F32),
                pltpu.SemaphoreType.DMA((12,)),
                pltpu.SemaphoreType.DMA,
                pltpu.SemaphoreType.DMA((100,)),
                pltpu.SemaphoreType.DMA((100,)),
            ],
            compiler_params=pltpu.CompilerParams(collective_id=0, has_side_effects=True, vmem_limit_bytes=VMEM_BYTES),
            name="tail",
        )(part, x_steps, vecs, w_o, w_fc, w_proj)
        return ys, k_new.reshape(key_buf.shape), v_new.reshape(val_buf.shape)

    return jax.shard_map(per_device, mesh=mesh, in_specs=in_specs, out_specs=out_specs, check_vma=False)
```

```python
import functools

import jax
import jax.numpy as jnp
from jax import lax
from jax.experimental import pallas as pl
from jax.experimental.pallas import tpu as pltpu
from jax.sharding import PartitionSpec as P

ROPE_BASE = 1000000.0
LN_EPS = 1e-5
NEG_BIG = -1e30
MESH = pl.DeviceIdType.MESH
F32 = jnp.float32
BF16 = jnp.bfloat16
VMEM_BYTES = 67043328


def one_hot_rows(size, inner):
    outer = size // inner
    row = lax.broadcasted_iota(jnp.int32, (size, size), 0)
    col = lax.broadcasted_iota(jnp.int32, (size, size), 1)
    source = lax.rem(row, outer) * inner + lax.div(row, outer)
    return jnp.where(col == source, 1.0, 0.0).astype(BF16)


def front_kernel(pos_ref, x_any, wq_any, wk_any, wv_any, gain_ref, shift_ref, bq_ref, bk_ref, bv_ref, cos_ref, sin_ref,
                 kc_any, vc_any,
                 part_ref, kout_any, vout_any,
                 x_buf, hid, wq_buf, wk_buf, wv_buf, acc, qkv, k_buf, v_buf,
                 x_sem, wq_sem, kv_sem, c_sem, out_sem, *, batch, heads, head_dim, steps, per):
    rows, width = x_buf.shape
    n_q = heads * head_dim
    bands, band = wq_buf.shape[0], wq_buf.shape[1]
    local = k_buf.shape[1]
    slots = local * lax.axis_size("sq")
    groups = batch // per
    half = heads // 2
    first = lax.axis_index("sq") * local
    leader = lax.axis_index("sq") == 0

    x_copy = pltpu.make_async_copy(x_any, x_buf, x_sem)
    x_copy.start()
    k_copy = pltpu.make_async_copy(wk_any, wk_buf, kv_sem.at[0])
    v_copy = pltpu.make_async_copy(wv_any, wv_buf, kv_sem.at[1])

    def q_copy(i):
        return pltpu.make_async_copy(wq_any.at[pl.ds(pl.multiple_of(i * band, band), band), :], wq_buf.at[i], wq_sem.at[i])

    def cache_in(i):
        at = pl.ds(i * per, per)
        return (pltpu.make_async_copy(kc_any.at[at], k_buf.at[at], c_sem.at[0, i]),
                pltpu.make_async_copy(vc_any.at[at], v_buf.at[at], c_sem.at[1, i]))

    def cache_out(i):
        at = pl.ds(i * per, per)
        return (pltpu.make_async_copy(k_buf.at[at], kout_any.at[at], out_sem.at[0, i]),
                pltpu.make_async_copy(v_buf.at[at], vout_any.at[at], out_sem.at[1, i]))

    gain = as_row(gain_ref)
    shift = as_row(shift_ref)
    x_copy.wait()
    k_copy.start()
    v_copy.start()
    for i in range(bands // 2):
        q_copy(i).start()

    def norm_rows(i, carry):
        at = pl.ds(pl.multiple_of(i * 16, 16), 16)
        vals = x_buf[at, :].astype(F32)
        mean = jnp.sum(vals, axis=-1, keepdims=True) * (1.0 / width)
        vals = vals - mean
        var = jnp.sum(vals * vals, axis=-1, keepdims=True) * (1.0 / width)
        hid[at, :] = (vals * lax.rsqrt(var + LN_EPS) * gain + shift).astype(BF16)
        return carry

    lax.fori_loop(0, rows // 16, norm_rows, 0, unroll=2)

    perm = one_hot_rows(rows, batch)
    cos_t = cos_ref[...]
    sin_t = sin_ref[...]

    def rotate(vals):
        return vals * cos_t + pltpu.roll(vals, head_dim // 2, 1) * sin_t

    def by_batch(vals):
        return jnp.dot(perm, vals.astype(BF16), preferred_element_type=F32)

    k_copy.wait()
    v_copy.wait()
    for i in range(bands // 2, bands):
        q_copy(i).start()
    k_new = jnp.dot(hid[...], wk_buf[...], preferred_element_type=F32) + as_row(bk_ref)
    v_new = jnp.dot(hid[...], wv_buf[...], preferred_element_type=F32) + as_row(bv_ref)
    qkv[heads] = by_batch(rotate(k_new.astype(BF16).astype(F32)))
    qkv[heads + 1] = by_batch(v_new)
    acc[...] = jnp.broadcast_to(as_row(bq_ref), acc.shape)

    def q_band(i, carry):
        q_copy(i).wait()

        @pl.when(i >= bands - groups // 2)
        def _():
            for j in range(2):
                for cp in cache_in(2 * (i - bands + groups // 2) + j):
                    cp.start()

        acc[...] += jnp.dot(hid[:, pl.ds(pl.multiple_of(i * band, band), band)], wq_buf[i], preferred_element_type=F32)
        return carry

    lax.fori_loop(0, bands, q_band, 0)

    for h in range(heads):
        vals = acc[:, h * head_dim:(h + 1) * head_dim]
        qkv[h] = by_batch(rotate(vals.astype(BF16).astype(F32)))

    scale = head_dim ** -0.5
    pair_rows = 2 * steps
    row = lax.broadcasted_iota(jnp.int32, (pair_rows, local), 0)
    slot = lax.broadcasted_iota(jnp.int32, (pair_rows, local), 1) + first
    step = lax.rem(row, steps)
    n_row = lax.broadcasted_iota(jnp.int32, (pair_rows, head_dim), 0)
    n_col = lax.broadcasted_iota(jnp.int32, (pair_rows, head_dim), 1)
    new_ok = ((lax.div(n_row, steps) == lax.div(n_col, steps)) & (lax.rem(n_col, steps) <= lax.rem(n_row, steps))
              & (n_col < pair_rows) & leader)[None]
    lane = n_col
    pad = jnp.zeros((head_dim - pair_rows, head_dim), F32)
    window = lax.broadcasted_iota(jnp.int32, (16, head_dim), 0)
    nt = (((1,), (1,)), ((), ()))

    def group(i, carry):
        for cp in cache_in(i):
            cp.wait()
        for pr in range(per // 2):
            b0 = i * per + 2 * pr
            rows_at = pl.ds(pl.multiple_of(i * (per * steps) + pair_rows * pr, pair_rows), pair_rows)
            pos0 = pos_ref[b0]
            pos1 = pos_ref[b0 + 1]
            cur = jnp.where(row < steps, pos0, pos1) + step
            if slots & (slots - 1):
                dist = lax.rem(lax.rem(cur - slot, slots) + slots, slots)
            else:
                dist = (cur - slot) & (slots - 1)
            old_ok = ((dist > step) & (dist <= cur))[None]
            query = qkv[0:heads, rows_at, :].reshape(heads * pair_rows, head_dim).astype(BF16)
            new_k = jnp.concatenate([qkv[heads, rows_at, :], pad], axis=0).astype(BF16)
            new_v = jnp.concatenate([qkv[heads + 1, rows_at, :], pad], axis=0).astype(BF16)
            shape = (heads, pair_rows, local)
            score0 = lax.dot_general(query, k_buf[b0], nt, preferred_element_type=F32).reshape(shape)
            score1 = lax.dot_general(query, k_buf[b0 + 1], nt, preferred_element_type=F32).reshape(shape)
            score = jnp.where(old_ok, jnp.where((row < steps)[None], score0, score1) * scale, NEG_BIG)
            shape = (heads, pair_rows, head_dim)
            score_n = lax.dot_general(query, new_k, nt, preferred_element_type=F32).reshape(shape) * scale
            score_n = jnp.where(new_ok, score_n, NEG_BIG)
            top = jnp.max(jnp.maximum(score_n, functools.reduce(
                jnp.maximum, [score[:, :, j:j + head_dim] for j in range(0, local, head_dim)])), axis=-1, keepdims=True)
            wts = jnp.where(old_ok, jnp.exp(score - top), 0.0)
            wts_n = jnp.where(new_ok, jnp.exp(score_n - top), 0.0)
            total = jnp.sum(wts_n + sum(wts[:, :, j:j + head_dim] for j in range(0, local, head_dim)), axis=-1, keepdims=True)
            wts = wts.reshape(heads * pair_rows, local).astype(BF16)
            wts_n = wts_n.reshape(heads * pair_rows, head_dim).astype(BF16)
            out0 = jnp.dot(wts, v_buf[b0], preferred_element_type=F32).reshape(shape)
            out1 = jnp.dot(wts, v_buf[b0 + 1], preferred_element_type=F32).reshape(shape)
            out_n = jnp.dot(wts_n, new_v, preferred_element_type=F32).reshape(shape)
            out = jnp.where((n_row < steps)[None], out0, out1) + out_n
            for core in range(2):
                part_ref[core, 0:half, rows_at, :] = out[core * half:(core + 1) * half]
                stat = jnp.zeros((pair_rows, head_dim), F32)
                for h in range(half):
                    stat = jnp.where(lane == h, top[core * half + h], stat)
                    stat = jnp.where(lane == head_dim // 2 + h, total[core * half + h], stat)
                part_ref[core, half, rows_at, :] = stat
        for b in range(per):
            lead = pos_ref[i * per + b] - first
            head_at = lax.rem(lead + slots, slots)

            @pl.when((head_at < local) | (head_at >= slots - steps))
            def _(b=b, head_at=head_at):
                for t in range(steps):
                    at = lax.rem(head_at + t, slots)

                    @pl.when(at < local)
                    def _(t=t, at=at):
                        start = pl.multiple_of(lax.div(at, 16) * 16, 16)
                        hit = window == at - start
                        for src, dst in ((heads, k_buf), (heads + 1, v_buf)):
                            fresh = qkv[src, pl.ds(i * (per * steps) + b * steps + t, 1), :]
                            old = dst[i * per + b, pl.ds(start, 16), :].astype(F32)
                            dst[i * per + b, pl.ds(start, 16), :] = jnp.where(hit, fresh, old).astype(BF16)

        for cp in cache_out(i):
            cp.start()
        return carry

    lax.fori_loop(0, groups, group, 0)
    for i in range(groups):
        for cp in cache_out(i):
            cp.wait()


def as_row(ref):
    return ref[...].astype(F32).reshape(1, ref.shape[0])


def merge_parts(parts, half, head_dim):
    stats = [p[half] for p in parts]
    top = functools.reduce(jnp.maximum, stats)
    scales = [jnp.exp(s - top) for s in stats]
    lane = lax.broadcasted_iota(jnp.int32, top.shape, 1)
    total = sum(s * pltpu.roll(f, head_dim // 2, 1) for s, f in zip(stats, scales))
    stat = jnp.where(lane < head_dim // 2, top, total)
    outs = []
    for h in range(half):
        outs.append(sum(p[h] * f[:, h:h + 1] for p, f in zip(parts, scales)))
    return outs, stat


def tail_kernel(part_ref, x_any, bo_ref, bpj_ref, gain_ref, shift_ref, bfc_ref, wo_any, wfc_any, wpj_any, y_ref,
                w_buf, x_buf, pair_in, m_part, x_in, a_own, a_in, a_full, o_part, o_in, x1_all, hid,
                g_own, g_in, g_full, p_part, p_in, y_all, bias_rows, w_sem, x_sem, send, recv, *, half, head_dim):
    steps, blk_b, cols = x_buf.shape
    blk = steps * blk_b
    n = 4
    width = 2 * n * cols
    core_cols = n * cols
    depth = wo_any.shape[0]
    ff = wpj_any.shape[0]
    sq = lax.axis_index("sq")
    y = lax.axis_index("tp")
    x = lax.div(sq, 2)
    c = lax.rem(sq, 2)
    mine = c * n + y
    my_col = pl.multiple_of(mine * cols, cols)
    half_col = pl.multiple_of(c * core_cols, core_cols)
    lo, hi = pl.ds(0, blk // 2), pl.ds(blk // 2, blk // 2)
    left, right = pl.ds(0, cols // 2), pl.ds(cols // 2, cols // 2)
    every = pl.ds(0, blk)
    all_cols = pl.ds(0, cols)
    partner = {"tp": y, "sq": 2 * x + 1 - c}

    def along_x(d):
        return {"tp": y, "sq": 2 * lax.rem(x + d, n) + c}

    def along_y(d):
        return {"tp": lax.rem(y + d, n), "sq": sq}

    ids = iter(range(1000))
    sent = []

    def push(src, dst, dev):
        i = next(ids)
        cp = pltpu.make_async_remote_copy(src_ref=src, dst_ref=dst, send_sem=send.at[i], recv_sem=recv.at[i],
                                          device_id=dev, device_id_type=MESH)
        cp.start()
        sent.append(cp)
        return cp

    order = (2, 1, 3, 0)

    def block_col(d):
        return pl.multiple_of(half_col + lax.rem(y + d, n) * cols, cols)

    wo_copy = [pltpu.make_async_copy(wo_any.at[:, pl.ds(block_col(d), cols)], w_buf.at[0, pl.ds(d * depth, depth)], w_sem.at[d])
               for d in range(n)]
    fc_copy = [pltpu.make_async_copy(wfc_any.at[:, pl.ds(pl.multiple_of(half_col + j * cols, cols), cols)], w_buf.at[1 + j],
                                     w_sem.at[n + j]) for j in range(n)]
    pj_copy = [pltpu.make_async_copy(wpj_any.at[:, pl.ds(block_col(d), cols)], w_buf.at[k], w_sem.at[2 * n + k])
               for k, d in enumerate(order)]
    x_copy = pltpu.make_async_copy(x_any.at[:, pl.ds(pl.multiple_of(x * blk_b, blk_b), blk_b), pl.ds(my_col, cols)], x_buf, x_sem)
    x_copy.start()
    for d in order:
        wo_copy[d].start()
    fc_copy[0].start()

    barrier = pltpu.get_barrier_semaphore()
    peers = [partner] + [along_x(d) for d in (1, 3)] + [along_y(d) for d in (1, 3)]
    for dev in peers:
        pl.semaphore_signal(barrier, inc=1, device_id=dev, device_id_type=MESH)
    for i, ref in enumerate((bo_ref, bpj_ref, bfc_ref, gain_ref, shift_ref)):
        bias_rows[8 * i:8 * i + 1, :] = as_row(ref)
    pl.semaphore_wait(barrier, len(peers))

    def ring_reduce(ready, half_of, inbox, along, fold):
        ready(2)
        rel_a = push(half_of(2, lo), inbox.at[0], along(1))
        rel_b = push(half_of(2, hi), inbox.at[1], along(3))
        ready(1)
        dir_b = push(half_of(1, hi), inbox.at[2], along(1))
        ready(3)
        dir_a = push(half_of(3, lo), inbox.at[3], along(3))
        rel_a.wait_recv()
        fold(1, lo, 0)
        sum_a = push(half_of(1, lo), inbox.at[4], along(1))
        rel_b.wait_recv()
        fold(3, hi, 1)
        sum_b = push(half_of(3, hi), inbox.at[5], along(3))
        ready(0)
        for cp in (dir_b, dir_a, sum_a, sum_b):
            cp.wait_recv()

    planes = range(half + 1)
    pairs = {}
    for d in order:
        at = pl.ds(pl.multiple_of(lax.rem(x + d, n) * blk, blk), blk)
        pairs[d] = push(part_ref.at[1 - c, :, at, :], pair_in.at[d], partner)
    fc_copy[1].start()

    def pair_merge(d):
        pairs[d].wait_recv()
        at = pl.ds(pl.multiple_of(lax.rem(x + d, n) * blk, blk), blk)
        outs, stat = merge_parts([[part_ref[c, h, at, :] for h in planes], [pair_in[d, h] for h in planes]], half, head_dim)
        for h in range(half):
            m_part[d, h] = outs[h]
        m_part[d, half] = stat

    def fold_parts(d, rows, i):
        outs, stat = merge_parts([[m_part[d, h, rows, :] for h in planes], [x_in[i, h] for h in planes]], half, head_dim)
        for h in range(half):
            m_part[d, h, rows, :] = outs[h]
        m_part[d, half, rows, :] = stat

    ring_reduce(pair_merge, lambda d, rows: m_part.at[d, :, rows], x_in, along_x, fold_parts)
    for rows, terms in ((lo, (3, 4)), (hi, (2, 5))):
        parts = [[m_part[0, h, rows, :] for h in planes]] + [[x_in[i, h] for h in planes] for i in terms]
        outs, stat = merge_parts(parts, half, head_dim)
        for h in range(half):
            denom = stat[:, head_dim // 2 + h:head_dim // 2 + h + 1]
            a_own[rows, h * head_dim:(h + 1) * head_dim] = (outs[h] / denom).astype(BF16).astype(F32)
    a_copy = push(a_own, a_in, partner)
    fc_copy[2].start()
    fc_copy[3].start()
    perm = one_hot_rows(blk, steps)
    a_cols = half * head_dim
    a_full[:, pl.ds(pl.multiple_of(c * a_cols, a_cols), a_cols)] = jnp.dot(
        perm, a_own[...].astype(BF16), preferred_element_type=F32).astype(BF16)
    a_copy.wait_recv()
    a_full[:, pl.ds(pl.multiple_of((1 - c) * a_cols, a_cols), a_cols)] = jnp.dot(
        perm, a_in[...].astype(BF16), preferred_element_type=F32).astype(BF16)

    def o_block(d):
        wo_copy[d].wait()
        o_part[d] = jnp.dot(a_full[...], w_buf[0, d * depth:(d + 1) * depth, :], preferred_element_type=F32)

    def fold_o(d, rows, i):
        o_part[d, rows, :] = o_part[d, rows, :] + o_in[i]

    ring_reduce(o_block, lambda d, rows: o_part.at[d, rows], o_in, along_y, fold_o)
    pj_copy[0].start()
    x_copy.wait()
    x_own = x_buf[...].astype(F32).reshape(blk, cols) + bias_rows[0:1, pl.ds(my_col, cols)]
    hb = blk // 2
    x1_all[mine, lo] = (x_own[:hb] + (o_part[0, lo] + (o_in[3] + o_in[4]))).astype(BF16).astype(F32)
    x1_all[mine, hi] = (x_own[hb:] + (o_part[0, hi] + (o_in[2] + o_in[5]))).astype(BF16).astype(F32)

    def x1_push(d, rows, dev):
        ref = x1_all.at[c * n + lax.rem(y + d, n), rows]
        return push(ref, ref, dev)

    p_lo = x1_push(0, lo, along_y(1))
    m_hi = x1_push(0, hi, along_y(3))
    p_hi = x1_push(0, hi, along_y(1))
    m_lo = x1_push(0, lo, along_y(3))
    fwd = [x1_push(0, every, partner)]
    p_lo.wait_recv()
    r_lo = x1_push(3, lo, along_y(1))
    m_hi.wait_recv()
    r_hi = x1_push(1, hi, along_y(3))
    p_hi.wait_recv()
    fwd.append(x1_push(3, every, partner))
    m_lo.wait_recv()
    fwd.append(x1_push(1, every, partner))
    r_lo.wait_recv()
    r_hi.wait_recv()
    fwd.append(x1_push(2, every, partner))
    for cp in fwd:
        cp.wait_recv()

    total = jnp.zeros((blk, 1), F32)
    for i in range(2 * n):
        total = total + jnp.sum(x1_all[i], axis=-1, keepdims=True)
    mean = total * (1.0 / width)
    total = jnp.zeros((blk, 1), F32)
    for i in range(2 * n):
        dev = x1_all[i] - mean
        total = total + jnp.sum(dev * dev, axis=-1, keepdims=True)
    inv = lax.rsqrt(total * (1.0 / width) + LN_EPS)
    for i in range(2 * n):
        at = slice(i * cols, (i + 1) * cols)
        gain = bias_rows[24:25, at]
        shift = bias_rows[32:33, at]
        hid[:, at] = ((x1_all[i] - mean) * inv * gain + shift).astype(BF16)

    own_ff = pl.multiple_of(c * (ff // 2), ff // 2)
    g_copy = []
    for j in range(n):
        fc_copy[j].wait()

        val = jnp.dot(hid[...], w_buf[1 + j], preferred_element_type=F32)
        ff_at = pl.ds(pl.multiple_of(own_ff + j * cols, cols), cols)
        val = jax.nn.gelu(val + bias_rows[16:17, ff_at], approximate=True).astype(BF16)
        g_own[j] = val.astype(F32)
        g_full[:, ff_at] = val
        g_copy.append(push(g_own.at[j], g_in.at[j], partner))
        if j < n - 1:
            pj_copy[j + 1].start()
    other_ff = pl.multiple_of((1 - c) * (ff // 2), ff // 2)
    for j in range(n):
        g_copy[j].wait_recv()
        g_full[:, pl.ds(pl.multiple_of(other_ff + j * cols, cols), cols)] = g_in[j].astype(BF16)

    def p_block(d):
        k = order.index(d)
        pj_copy[k].wait()

        p_part[d] = jnp.dot(g_full[...], w_buf[k], preferred_element_type=F32)

    def fold_p(d, rows, i):
        p_part[d, rows, :] = p_part[d, rows, :] + p_in[i]

    ring_reduce(p_block, lambda d, rows: p_part.at[d, rows], p_in, along_y, fold_p)
    bias = bias_rows[8:9, pl.ds(my_col, cols)]
    y_all[x, mine, lo] = (x1_all[mine, lo] + (p_part[0, lo] + (p_in[3] + p_in[4])) + bias).astype(BF16).astype(F32)
    y_all[x, mine, hi] = (x1_all[mine, hi] + (p_part[0, hi] + (p_in[2] + p_in[5])) + bias).astype(BF16).astype(F32)

    def unit(dx, dy, rows=every, at=all_cols):
        return y_all.at[lax.rem(x + dx, n), c * n + lax.rem(y + dy, n), rows, at]

    def relay(dx, dy, dev, rows=every, at=all_cols):
        ref = unit(dx, dy, rows, at)
        return push(ref, ref, dev)

    fwd = []

    def forward(dx, dy):
        fwd.append(relay(dx, dy, partner))

    xp, xm, yp, ym = along_x(1), along_x(3), along_y(1), along_y(3)
    own = {}
    for first_half in (True, False):
        for key, dev in (("xp", xp), ("xm", xm), ("yp", yp), ("ym", ym)):
            own[key, first_half] = relay(0, 0, dev, at=left if (key[1] == "p") == first_half else right)
    forward(0, 0)
    own["xp", True].wait_recv()
    r_xp = relay(3, 0, xp, at=left)
    own["xm", True].wait_recv()
    r_xm = relay(1, 0, xm, at=right)
    own["yp", True].wait_recv()
    r_yp = relay(0, 3, yp, at=left)
    own["ym", True].wait_recv()
    r_ym = relay(0, 1, ym, at=right)
    own["xp", False].wait_recv()
    a_yp, a_ym = relay(3, 0, yp, rows=lo), relay(3, 0, ym, rows=lo)
    own["xm", False].wait_recv()
    b_yp, b_ym = relay(1, 0, yp, rows=lo), relay(1, 0, ym, rows=lo)
    own["yp", False].wait_recv()
    a_xp, a_xm = relay(0, 3, xp, rows=hi), relay(0, 3, xm, rows=hi)
    own["ym", False].wait_recv()
    b_xp, b_xm = relay(0, 1, xp, rows=hi), relay(0, 1, xm, rows=hi)
    for d in ((3, 0), (1, 0), (0, 3), (0, 1)):
        forward(*d)
    r_xp.wait_recv()
    c_yp, c_ym = relay(2, 0, yp, lo, left), relay(2, 0, ym, lo, left)
    r_xm.wait_recv()
    d_yp, d_ym = relay(2, 0, yp, lo, right), relay(2, 0, ym, lo, right)
    r_yp.wait_recv()
    c_xp, c_xm = relay(0, 2, xp, hi, left), relay(0, 2, xm, hi, left)
    r_ym.wait_recv()
    d_xp, d_xm = relay(0, 2, xp, hi, right), relay(0, 2, xm, hi, right)
    forward(2, 0)
    forward(0, 2)
    late = []
    for cp, dx, dy, dev, rows, at in ((a_yp, 3, 3, yp, lo, left), (a_ym, 3, 1, ym, lo, right),
                                      (b_yp, 1, 3, yp, lo, left), (b_ym, 1, 1, ym, lo, right),
                                      (a_xp, 3, 3, xp, hi, left), (a_xm, 1, 3, xm, hi, right),
                                      (b_xp, 3, 1, xp, hi, left), (b_xm, 1, 1, xm, hi, right)):
        cp.wait_recv()
        late.append(relay(dx, dy, dev, rows, at))
    for d in ((3, 3), (3, 1), (1, 3), (1, 1)):
        forward(*d)
    for cp, dx, dy, dev, rows, at in ((c_yp, 2, 3, yp, lo, left), (d_ym, 2, 1, ym, lo, right),
                                      (c_xp, 3, 2, xp, hi, left), (d_xm, 1, 2, xm, hi, right)):
        cp.wait_recv()
        late.append(relay(dx, dy, dev, rows, at))
    for cp in (c_ym, d_yp, c_xm, d_xp):
        cp.wait_recv()
    for cp in late[:8]:
        cp.wait_recv()
    for d in ((3, 2), (1, 2), (2, 3), (2, 1)):
        forward(*d)
    for cp in late[8:]:
        cp.wait_recv()
    forward(2, 2)
    for cp in fwd:
        cp.wait_recv()
    for s in range(steps):
        for xb in range(0, n, 2):
            for i in range(2 * n):
                block = jnp.concatenate([y_all[xb, i, s * blk_b:(s + 1) * blk_b, :],
                                         y_all[xb + 1, i, s * blk_b:(s + 1) * blk_b, :]], axis=0)
                y_ref[s, xb * blk_b:(xb + 2) * blk_b, i * cols:(i + 1) * cols] = block.astype(BF16)
    for cp in sent:
        cp.wait_send()


def solution(mesh):
    n_sq = mesh.shape["sq"]
    n_y = mesh.shape["tp"]
    n_x = n_sq // 2
    act_spec = P(None, "dp", None)
    cache_spec = P("dp", "sq", "tp", None)
    col_spec = P(None, "tp")
    row_spec = P("tp", None)
    vec_spec = P("tp")
    rep_spec = P(None)
    in_specs = (act_spec, P("dp"), cache_spec, cache_spec, col_spec, vec_spec, col_spec, vec_spec,
                col_spec, vec_spec, row_spec, rep_spec, rep_spec, rep_spec, rep_spec, rep_spec,
                col_spec, vec_spec, row_spec, rep_spec)
    out_specs = (act_spec, cache_spec, cache_spec)
    vmem = pl.BlockSpec(memory_space=pltpu.VMEM)
    hbm = pl.BlockSpec(memory_space=pl.ANY)

    def per_device(x_steps, positions, key_buf, val_buf, w_q, b_q, w_k, b_k, w_v, b_v, w_o, b_o,
                   ln1_gain, ln1_bias, ln2_gain, ln2_bias, w_fc, b_fc, w_proj, b_proj):
        steps, batch, width = x_steps.shape
        local, head_dim = key_buf.shape[1], key_buf.shape[3]
        rows = steps * batch
        heads = w_q.shape[1] // head_dim
        half = heads // 2
        half_dim = head_dim // 2
        inv_freq = jnp.power(jnp.float32(ROPE_BASE), -2.0 * jnp.arange(half_dim, dtype=F32) / head_dim)
        inv_freq = jnp.concatenate([inv_freq, inv_freq])[None, None, :]
        sign = jnp.where(jnp.arange(head_dim) < half_dim, -1.0, 1.0).astype(F32)
        cur = positions[None, :, None] + jnp.arange(steps, dtype=jnp.int32)[:, None, None]
        angle = cur.astype(F32) * inv_freq
        cos_t = jnp.cos(angle).reshape(rows, head_dim)
        sin_t = (jnp.sin(angle) * sign).reshape(rows, head_dim)

        per, bands = 4, 6
        groups = batch // per
        smem = pl.BlockSpec(memory_space=pltpu.SMEM)
        part, k_new, v_new = pl.pallas_call(
            functools.partial(front_kernel, batch=batch, heads=heads, head_dim=head_dim, steps=steps, per=per),
            out_shape=(jax.ShapeDtypeStruct((2, half + 1, rows, head_dim), F32),
                       jax.ShapeDtypeStruct((batch, local, head_dim), BF16),
                       jax.ShapeDtypeStruct((batch, local, head_dim), BF16)),
            in_specs=[smem] + [hbm] * 4 + [vmem] * 7 + [hbm] * 2,
            out_specs=(vmem, hbm, hbm),
            scratch_shapes=[
                pltpu.VMEM((rows, width), BF16),
                pltpu.VMEM((rows, width), BF16),
                pltpu.VMEM((bands, width // bands, heads * head_dim), BF16),
                pltpu.VMEM((width, head_dim), BF16),
                pltpu.VMEM((width, head_dim), BF16),
                pltpu.VMEM((rows, heads * head_dim), F32),
                pltpu.VMEM((heads + 2, rows, head_dim), F32),
                pltpu.VMEM((batch, local, head_dim), BF16),
                pltpu.VMEM((batch, local, head_dim), BF16),
                pltpu.SemaphoreType.DMA,
                pltpu.SemaphoreType.DMA((bands,)),
                pltpu.SemaphoreType.DMA((2,)),
                pltpu.SemaphoreType.DMA((2, groups)),
                pltpu.SemaphoreType.DMA((2, groups)),
            ],
            compiler_params=pltpu.CompilerParams(vmem_limit_bytes=VMEM_BYTES),
            name="front",
        )(positions, x_steps.reshape(rows, width), w_q, w_k, w_v, ln1_gain, ln1_bias, b_q, b_k, b_v, cos_t, sin_t,
          key_buf.reshape(batch, local, head_dim), val_buf.reshape(batch, local, head_dim))

        cols = width // (2 * n_y)
        core_cols = width // 2
        blk_b = batch // n_x
        blk = blk_b * steps
        ys = pl.pallas_call(
            functools.partial(tail_kernel, half=half, head_dim=head_dim),
            out_shape=jax.ShapeDtypeStruct((steps, batch, width), BF16),
            in_specs=[vmem, hbm] + [vmem] * 5 + [hbm] * 3,
            out_specs=vmem,
            scratch_shapes=[
                pltpu.VMEM((5, width, cols), BF16),
                pltpu.VMEM((steps, blk_b, cols), BF16),
                pltpu.VMEM((4, half + 1, blk, head_dim), F32),
                pltpu.VMEM((4, half + 1, blk, head_dim), F32),
                pltpu.VMEM((6, half + 1, blk // 2, head_dim), F32),
                pltpu.VMEM((blk, half * head_dim), F32),
                pltpu.VMEM((blk, half * head_dim), F32),
                pltpu.VMEM((blk, heads * head_dim), BF16),
                pltpu.VMEM((4, blk, cols), F32),
                pltpu.VMEM((6, blk // 2, cols), F32),
                pltpu.VMEM((8, blk, cols), F32),
                pltpu.VMEM((blk, width), BF16),
                pltpu.VMEM((4, blk, cols), F32),
                pltpu.VMEM((4, blk, cols), F32),
                pltpu.VMEM((blk, w_proj.shape[0]), BF16),
                pltpu.VMEM((4, blk, cols), F32),
                pltpu.VMEM((6, blk // 2, cols), F32),
                pltpu.VMEM((4, 8, blk, cols), F32),
                pltpu.VMEM((40, width), F32),
                pltpu.SemaphoreType.DMA((12,)),
                pltpu.SemaphoreType.DMA,
                pltpu.SemaphoreType.DMA((100,)),
                pltpu.SemaphoreType.DMA((100,)),
            ],
            compiler_params=pltpu.CompilerParams(collective_id=0, has_side_effects=True, vmem_limit_bytes=VMEM_BYTES),
            name="tail",
        )(part, x_steps, b_o, b_proj, ln2_gain, ln2_bias, b_fc, w_o, w_fc, w_proj)
        return ys, k_new.reshape(key_buf.shape), v_new.reshape(val_buf.shape)

    return jax.shard_map(per_device, mesh=mesh, in_specs=in_specs, out_specs=out_specs, check_vma=False)
```

```python
import functools

import jax
import jax.numpy as jnp
from jax import lax
from jax.experimental import pallas as pl
from jax.experimental.pallas import tpu as pltpu
from jax.sharding import PartitionSpec as P

ROPE_BASE = 1000000.0
LN_EPS = 1e-5
NEG_BIG = -1e30
MESH = pl.DeviceIdType.MESH
F32 = jnp.float32
BF16 = jnp.bfloat16
VMEM_BYTES = 67043328


def one_hot_rows(size, inner):
    outer = size // inner
    row = lax.broadcasted_iota(jnp.int32, (size, size), 0)
    col = lax.broadcasted_iota(jnp.int32, (size, size), 1)
    source = lax.rem(row, outer) * inner + lax.div(row, outer)
    return jnp.where(col == source, 1.0, 0.0).astype(BF16)


def front_kernel(pos_ref, x_any, wq_any, wk_any, wv_any, gain_ref, shift_ref, bq_ref, bk_ref, bv_ref, cos_ref, sin_ref,
                 kc_any, vc_any,
                 part_ref, kout_any, vout_any,
                 x_buf, hid, wq_buf, wk_buf, wv_buf, acc, qkv, k_buf, v_buf, s_buf, n_buf, p_buf,
                 x_sem, wq_sem, kv_sem, c_sem, out_sem, *, batch, heads, head_dim, steps, per):
    rows, width = x_buf.shape
    n_q = heads * head_dim
    bands, band = wq_buf.shape[0], wq_buf.shape[1]
    local = k_buf.shape[1]
    slots = local * lax.axis_size("sq")
    groups = batch // per
    half = heads // 2
    first = lax.axis_index("sq") * local
    leader = lax.axis_index("sq") == 0

    def x_copy(i):
        at = pl.ds(pl.multiple_of(i * 16, 16), 16)
        return pltpu.make_async_copy(x_any.at[at], x_buf.at[at], x_sem.at[i])

    for i in range(rows // 16):
        x_copy(i).start()
    k_copy = pltpu.make_async_copy(wk_any, wk_buf, kv_sem.at[0])
    v_copy = pltpu.make_async_copy(wv_any, wv_buf, kv_sem.at[1])

    def q_copy(i):
        return pltpu.make_async_copy(wq_any.at[pl.ds(pl.multiple_of(i * band, band), band), :], wq_buf.at[i], wq_sem.at[i])

    def cache_in(i):
        at = pl.ds(i * per, per)
        return (pltpu.make_async_copy(kc_any.at[at], k_buf.at[at], c_sem.at[0, i]),
                pltpu.make_async_copy(vc_any.at[at], v_buf.at[at], c_sem.at[1, i]))

    def cache_out(i):
        at = pl.ds(i * per, per)
        return (pltpu.make_async_copy(k_buf.at[at], kout_any.at[at], out_sem.at[0, i]),
                pltpu.make_async_copy(v_buf.at[at], vout_any.at[at], out_sem.at[1, i]))

    gain = as_row(gain_ref)
    shift = as_row(shift_ref)
    k_copy.start()
    v_copy.start()
    q_copy(0).start()

    def norm_rows(i, carry):
        x_copy(i).wait()
        at = pl.ds(pl.multiple_of(i * 16, 16), 16)
        vals = x_buf[at, :].astype(F32)
        mean = jnp.sum(vals, axis=-1, keepdims=True) * (1.0 / width)
        vals = vals - mean
        var = jnp.sum(vals * vals, axis=-1, keepdims=True) * (1.0 / width)
        hid[at, :] = (vals * lax.rsqrt(var + LN_EPS) * gain + shift).astype(BF16)
        return carry

    lax.fori_loop(0, rows // 16, norm_rows, 0, unroll=2)
    for i in range(1, bands // 2):
        q_copy(i).start()

    perm = one_hot_rows(rows, batch)
    cos_t = cos_ref[...]
    sin_t = sin_ref[...]

    def rotate(vals):
        return vals * cos_t + pltpu.roll(vals, head_dim // 2, 1) * sin_t

    def by_batch(vals):
        return jnp.dot(perm, vals.astype(BF16), preferred_element_type=F32)

    k_copy.wait()
    v_copy.wait()
    for i in range(bands // 2, bands):
        q_copy(i).start()
    k_new = jnp.dot(hid[...], wk_buf[...], preferred_element_type=F32) + as_row(bk_ref)
    v_new = jnp.dot(hid[...], wv_buf[...], preferred_element_type=F32) + as_row(bv_ref)
    qkv[heads] = by_batch(rotate(k_new.astype(BF16).astype(F32)))
    qkv[heads + 1] = by_batch(v_new)
    acc[...] = jnp.broadcast_to(as_row(bq_ref), acc.shape)

    def q_band(i, carry):
        q_copy(i).wait()

        @pl.when(i >= bands - groups // 2)
        def _():
            for j in range(2):
                for cp in cache_in(2 * (i - bands + groups // 2) + j):
                    cp.start()

        acc[...] += jnp.dot(hid[:, pl.ds(pl.multiple_of(i * band, band), band)], wq_buf[i], preferred_element_type=F32)
        return carry

    lax.fori_loop(0, bands, q_band, 0)

    for h in range(heads):
        vals = acc[:, h * head_dim:(h + 1) * head_dim]
        qkv[h] = by_batch(rotate(vals.astype(BF16).astype(F32)))

    scale = head_dim ** -0.5
    pair_rows = 2 * steps
    row = lax.broadcasted_iota(jnp.int32, (pair_rows, local), 0)
    slot = lax.broadcasted_iota(jnp.int32, (pair_rows, local), 1) + first
    step = lax.rem(row, steps)
    n_row = lax.broadcasted_iota(jnp.int32, (pair_rows, head_dim), 0)
    n_col = lax.broadcasted_iota(jnp.int32, (pair_rows, head_dim), 1)
    new_ok = ((lax.div(n_row, steps) == lax.div(n_col, steps)) & (lax.rem(n_col, steps) <= lax.rem(n_row, steps))
              & (n_col < pair_rows) & leader)[None]
    lane = n_col
    pad = jnp.zeros((head_dim - pair_rows, head_dim), F32)
    window = lax.broadcasted_iota(jnp.int32, (16, head_dim), 0)
    nt = (((1,), (1,)), ((), ()))

    def group(i, carry):
        for cp in cache_in(i):
            cp.wait()
        s_shape = (heads, pair_rows, local)
        o_shape = (heads, pair_rows, head_dim)

        def rows_of(pr):
            return pl.ds(pl.multiple_of(i * (per * steps) + pair_rows * pr, pair_rows), pair_rows)

        def mask_of(pr):
            b0 = i * per + 2 * pr
            cur = jnp.where(row < steps, pos_ref[b0], pos_ref[b0 + 1]) + step
            if slots & (slots - 1):
                dist = lax.rem(lax.rem(cur - slot, slots) + slots, slots)
            else:
                dist = (cur - slot) & (slots - 1)
            return ((dist > step) & (dist <= cur))[None]

        for pr in range(per // 2):
            b0 = i * per + 2 * pr
            query = qkv[0:heads, rows_of(pr), :].reshape(heads * pair_rows, head_dim).astype(BF16)
            new_k = jnp.concatenate([qkv[heads, rows_of(pr), :], pad], axis=0).astype(BF16)
            score0 = lax.dot_general(query, k_buf[b0], nt, preferred_element_type=F32).reshape(s_shape)
            score1 = lax.dot_general(query, k_buf[b0 + 1], nt, preferred_element_type=F32).reshape(s_shape)
            s_buf[pr] = jnp.where(mask_of(pr), jnp.where((row < steps)[None], score0, score1) * scale, NEG_BIG)
            score_n = lax.dot_general(query, new_k, nt, preferred_element_type=F32).reshape(o_shape) * scale
            n_buf[pr] = jnp.where(new_ok, score_n, NEG_BIG)
        for pr in range(per // 2):
            score = s_buf[pr]
            score_n = n_buf[pr]
            top = jnp.max(jnp.maximum(score_n, functools.reduce(
                jnp.maximum, [score[:, :, j:j + head_dim] for j in range(0, local, head_dim)])), axis=-1, keepdims=True)
            wts = jnp.where(mask_of(pr), jnp.exp(score - top), 0.0)
            wts_n = jnp.where(new_ok, jnp.exp(score_n - top), 0.0)
            total = jnp.sum(wts_n + sum(wts[:, :, j:j + head_dim] for j in range(0, local, head_dim)), axis=-1, keepdims=True)
            p_buf[pr, :, 0:local] = wts.reshape(heads * pair_rows, local).astype(BF16)
            p_buf[pr, :, local:] = wts_n.reshape(heads * pair_rows, head_dim).astype(BF16)
            for core in range(2):
                stat = jnp.zeros((pair_rows, head_dim), F32)
                for h in range(half):
                    stat = jnp.where(lane == h, top[core * half + h], stat)
                    stat = jnp.where(lane == head_dim // 2 + h, total[core * half + h], stat)
                part_ref[core, half, rows_of(pr), :] = stat
        for pr in range(per // 2):
            b0 = i * per + 2 * pr
            new_v = jnp.concatenate([qkv[heads + 1, rows_of(pr), :], pad], axis=0).astype(BF16)
            out0 = jnp.dot(p_buf[pr, :, 0:local], v_buf[b0], preferred_element_type=F32).reshape(o_shape)
            out1 = jnp.dot(p_buf[pr, :, 0:local], v_buf[b0 + 1], preferred_element_type=F32).reshape(o_shape)
            out_n = jnp.dot(p_buf[pr, :, local:], new_v, preferred_element_type=F32).reshape(o_shape)
            out = jnp.where((n_row < steps)[None], out0, out1) + out_n
            for core in range(2):
                part_ref[core, 0:half, rows_of(pr), :] = out[core * half:(core + 1) * half]
        for b in range(per):
            lead = pos_ref[i * per + b] - first
            head_at = lax.rem(lead + slots, slots)

            @pl.when((head_at < local) | (head_at >= slots - steps))
            def _(b=b, head_at=head_at):
                for t in range(steps):
                    at = lax.rem(head_at + t, slots)

                    @pl.when(at < local)
                    def _(t=t, at=at):
                        start = pl.multiple_of(lax.div(at, 16) * 16, 16)
                        hit = window == at - start
                        for src, dst in ((heads, k_buf), (heads + 1, v_buf)):
                            fresh = qkv[src, pl.ds(i * (per * steps) + b * steps + t, 1), :]
                            old = dst[i * per + b, pl.ds(start, 16), :].astype(F32)
                            dst[i * per + b, pl.ds(start, 16), :] = jnp.where(hit, fresh, old).astype(BF16)

        for cp in cache_out(i):
            cp.start()
        return carry

    lax.fori_loop(0, groups, group, 0)
    for i in range(groups):
        for cp in cache_out(i):
            cp.wait()


def as_row(ref):
    return ref[...].astype(F32).reshape(1, ref.shape[0])


def merge_parts(parts, half, head_dim):
    stats = [p[half] for p in parts]
    top = functools.reduce(jnp.maximum, stats)
    scales = [jnp.exp(s - top) for s in stats]
    lane = lax.broadcasted_iota(jnp.int32, top.shape, 1)
    total = sum(s * pltpu.roll(f, head_dim // 2, 1) for s, f in zip(stats, scales))
    stat = jnp.where(lane < head_dim // 2, top, total)
    outs = []
    for h in range(half):
        outs.append(sum(p[h] * f[:, h:h + 1] for p, f in zip(parts, scales)))
    return outs, stat


def tail_kernel(part_ref, x_any, bo_ref, bpj_ref, gain_ref, shift_ref, bfc_ref, wo_any, wfc_any, wpj_any, y_ref,
                w_buf, x_buf, pair_in, m_part, x_in, a_own, a_in, a_full, o_part, o_in, x1_all, hid,
                g_own, g_in, g_full, p_part, p_in, y_all, bias_rows, w_ext, w_sem, x_sem, send, recv, *, half, head_dim):
    steps, blk_b, cols = x_buf.shape
    blk = steps * blk_b
    n = 4
    width = 2 * n * cols
    core_cols = n * cols
    depth = wo_any.shape[0]
    ff = wpj_any.shape[0]
    sq = lax.axis_index("sq")
    y = lax.axis_index("tp")
    x = lax.div(sq, 2)
    c = lax.rem(sq, 2)
    mine = c * n + y
    my_col = pl.multiple_of(mine * cols, cols)
    half_col = pl.multiple_of(c * core_cols, core_cols)
    lo, hi = pl.ds(0, blk // 2), pl.ds(blk // 2, blk // 2)
    left, right = pl.ds(0, cols // 2), pl.ds(cols // 2, cols // 2)
    every = pl.ds(0, blk)
    all_cols = pl.ds(0, cols)
    partner = {"tp": y, "sq": 2 * x + 1 - c}

    def along_x(d):
        return {"tp": y, "sq": 2 * lax.rem(x + d, n) + c}

    def along_y(d):
        return {"tp": lax.rem(y + d, n), "sq": sq}

    ids = iter(range(1000))
    sent = []

    def push(src, dst, dev):
        i = next(ids)
        cp = pltpu.make_async_remote_copy(src_ref=src, dst_ref=dst, send_sem=send.at[i], recv_sem=recv.at[i],
                                          device_id=dev, device_id_type=MESH)
        cp.start()
        sent.append(cp)
        return cp

    order = (2, 1, 3, 0)

    def block_col(d):
        return pl.multiple_of(half_col + lax.rem(y + d, n) * cols, cols)

    wo_copy = [pltpu.make_async_copy(wo_any.at[:, pl.ds(block_col(d), cols)], w_buf.at[0, pl.ds(d * depth, depth)], w_sem.at[d])
               for d in range(n)]
    fc_copy = [pltpu.make_async_copy(wfc_any.at[:, pl.ds(pl.multiple_of(half_col + j * cols, cols), cols)], w_buf.at[1 + j],
                                     w_sem.at[n + j]) for j in range(n)]
    pj_copy = [pltpu.make_async_copy(wpj_any.at[:, pl.ds(block_col(d), cols)], w_buf.at[k], w_sem.at[2 * n + k])
               for k, d in enumerate(order)]
    hc = cols // 2
    pj_copy[1] = pltpu.make_async_copy(wpj_any.at[:, pl.ds(pl.multiple_of(block_col(1) + hc, hc), hc)], w_buf.at[1, :, pl.ds(0, hc)],
                                       w_sem.at[2 * n + 1])
    ext_copy = pltpu.make_async_copy(wpj_any.at[:, pl.ds(block_col(1), hc)], w_ext, w_sem.at[3 * n])
    x_copy = pltpu.make_async_copy(x_any.at[:, pl.ds(pl.multiple_of(x * blk_b, blk_b), blk_b), pl.ds(my_col, cols)], x_buf, x_sem)
    x_copy.start()
    for d in order:
        wo_copy[d].start()
    fc_copy[0].start()

    barrier = pltpu.get_barrier_semaphore()
    peers = [partner] + [along_x(d) for d in (1, 3)] + [along_y(d) for d in (1, 3)]
    for dev in peers:
        pl.semaphore_signal(barrier, inc=1, device_id=dev, device_id_type=MESH)
    for i, ref in enumerate((bo_ref, bpj_ref, bfc_ref, gain_ref, shift_ref)):
        bias_rows[8 * i:8 * i + 1, :] = as_row(ref)
    pl.semaphore_wait(barrier, len(peers))

    def ring_reduce(ready, half_of, inbox, along, fold):
        ready(2)
        rel_a = push(half_of(2, lo), inbox.at[0], along(1))
        rel_b = push(half_of(2, hi), inbox.at[1], along(3))
        ready(1)
        dir_b = push(half_of(1, hi), inbox.at[2], along(1))
        ready(3)
        dir_a = push(half_of(3, lo), inbox.at[3], along(3))
        rel_a.wait_recv()
        fold(1, lo, 0)
        sum_a = push(half_of(1, lo), inbox.at[4], along(1))
        rel_b.wait_recv()
        fold(3, hi, 1)
        sum_b = push(half_of(3, hi), inbox.at[5], along(3))
        ready(0)
        for cp in (dir_b, dir_a, sum_a, sum_b):
            cp.wait_recv()

    planes = range(half + 1)
    pairs = {}
    for d in order:
        at = pl.ds(pl.multiple_of(lax.rem(x + d, n) * blk, blk), blk)
        pairs[d] = push(part_ref.at[1 - c, :, at, :], pair_in.at[d], partner)
    fc_copy[1].start()

    def pair_merge(d):
        pairs[d].wait_recv()
        at = pl.ds(pl.multiple_of(lax.rem(x + d, n) * blk, blk), blk)
        outs, stat = merge_parts([[part_ref[c, h, at, :] for h in planes], [pair_in[d, h] for h in planes]], half, head_dim)
        for h in range(half):
            m_part[d, h] = outs[h]
        m_part[d, half] = stat

    def fold_parts(d, rows, i):
        outs, stat = merge_parts([[m_part[d, h, rows, :] for h in planes], [x_in[i, h] for h in planes]], half, head_dim)
        for h in range(half):
            m_part[d, h, rows, :] = outs[h]
        m_part[d, half, rows, :] = stat

    ring_reduce(pair_merge, lambda d, rows: m_part.at[d, :, rows], x_in, along_x, fold_parts)
    for rows, terms in ((lo, (3, 4)), (hi, (2, 5))):
        parts = [[m_part[0, h, rows, :] for h in planes]] + [[x_in[i, h] for h in planes] for i in terms]
        outs, stat = merge_parts(parts, half, head_dim)
        for h in range(half):
            denom = stat[:, head_dim // 2 + h:head_dim // 2 + h + 1]
            a_own[rows, h * head_dim:(h + 1) * head_dim] = (outs[h] / denom).astype(BF16).astype(F32)
    a_copy = push(a_own, a_in, partner)
    fc_copy[2].start()
    fc_copy[3].start()
    perm = one_hot_rows(blk, steps)
    a_cols = half * head_dim
    a_full[:, pl.ds(pl.multiple_of(c * a_cols, a_cols), a_cols)] = jnp.dot(
        perm, a_own[...].astype(BF16), preferred_element_type=F32).astype(BF16)
    a_copy.wait_recv()
    a_full[:, pl.ds(pl.multiple_of((1 - c) * a_cols, a_cols), a_cols)] = jnp.dot(
        perm, a_in[...].astype(BF16), preferred_element_type=F32).astype(BF16)

    def o_block(d):
        wo_copy[d].wait()
        o_part[d] = jnp.dot(a_full[...], w_buf[0, d * depth:(d + 1) * depth, :], preferred_element_type=F32)

    def fold_o(d, rows, i):
        o_part[d, rows, :] = o_part[d, rows, :] + o_in[i]

    ring_reduce(o_block, lambda d, rows: o_part.at[d, rows], o_in, along_y, fold_o)
    pj_copy[0].start()
    ext_copy.start()
    x_copy.wait()
    x_own = x_buf[...].astype(F32).reshape(blk, cols) + bias_rows[0:1, pl.ds(my_col, cols)]
    hb = blk // 2
    x1_all[mine, lo] = (x_own[:hb] + (o_part[0, lo] + (o_in[3] + o_in[4]))).astype(BF16).astype(F32)
    x1_all[mine, hi] = (x_own[hb:] + (o_part[0, hi] + (o_in[2] + o_in[5]))).astype(BF16).astype(F32)

    def x1_push(d, rows, dev):
        ref = x1_all.at[c * n + lax.rem(y + d, n), rows]
        return push(ref, ref, dev)

    p_lo = x1_push(0, lo, along_y(1))
    m_hi = x1_push(0, hi, along_y(3))
    p_hi = x1_push(0, hi, along_y(1))
    m_lo = x1_push(0, lo, along_y(3))
    fwd = [x1_push(0, every, partner)]
    p_lo.wait_recv()
    r_lo = x1_push(3, lo, along_y(1))
    m_hi.wait_recv()
    r_hi = x1_push(1, hi, along_y(3))
    p_hi.wait_recv()
    fwd.append(x1_push(3, every, partner))
    m_lo.wait_recv()
    fwd.append(x1_push(1, every, partner))
    r_lo.wait_recv()
    r_hi.wait_recv()
    fwd.append(x1_push(2, every, partner))
    for cp in fwd:
        cp.wait_recv()

    total = jnp.zeros((blk, 1), F32)
    for i in range(2 * n):
        total = total + jnp.sum(x1_all[i], axis=-1, keepdims=True)
    mean = total * (1.0 / width)
    total = jnp.zeros((blk, 1), F32)
    for i in range(2 * n):
        dev = x1_all[i] - mean
        total = total + jnp.sum(dev * dev, axis=-1, keepdims=True)
    inv = lax.rsqrt(total * (1.0 / width) + LN_EPS)
    for i in range(2 * n):
        at = slice(i * cols, (i + 1) * cols)
        gain = bias_rows[24:25, at]
        shift = bias_rows[32:33, at]
        hid[:, at] = ((x1_all[i] - mean) * inv * gain + shift).astype(BF16)

    own_ff = pl.multiple_of(c * (ff // 2), ff // 2)
    g_copy = []
    for j in range(n):
        fc_copy[j].wait()

        val = jnp.dot(hid[...], w_buf[1 + j], preferred_element_type=F32)
        ff_at = pl.ds(pl.multiple_of(own_ff + j * cols, cols), cols)
        val = jax.nn.gelu(val + bias_rows[16:17, ff_at], approximate=True).astype(BF16)
        g_own[j] = val.astype(F32)
        g_full[:, ff_at] = val
        g_copy.append(push(g_own.at[j], g_in.at[j], partner))
        if j < n - 1:
            pj_copy[j + 1].start()
    other_ff = pl.multiple_of((1 - c) * (ff // 2), ff // 2)

    def p_block(d):
        k = order.index(d)
        pj_copy[k].wait()
        if k == 0:
            own_rows, other_rows = pl.ds(own_ff, ff // 2), pl.ds(other_ff, ff // 2)
            p_part[d] = jnp.dot(g_full[:, own_rows], w_buf[k, own_rows, :], preferred_element_type=F32)
            for j in range(n):
                g_copy[j].wait_recv()
                g_full[:, pl.ds(pl.multiple_of(other_ff + j * cols, cols), cols)] = g_in[j].astype(BF16)
            p_part[d] = p_part[d] + jnp.dot(g_full[:, other_rows], w_buf[k, other_rows, :], preferred_element_type=F32)
        elif k == 1:
            ext_copy.wait()
            p_part[d, :, 0:hc] = jnp.dot(g_full[...], w_ext[...], preferred_element_type=F32)
            p_part[d, :, hc:] = jnp.dot(g_full[...], w_buf[k, :, 0:hc], preferred_element_type=F32)
        else:
            p_part[d] = jnp.dot(g_full[...], w_buf[k], preferred_element_type=F32)

    def fold_p(d, rows, i):
        p_part[d, rows, :] = p_part[d, rows, :] + p_in[i]

    ring_reduce(p_block, lambda d, rows: p_part.at[d, rows], p_in, along_y, fold_p)
    bias = bias_rows[8:9, pl.ds(my_col, cols)]
    y_all[x, mine, lo] = (x1_all[mine, lo] + (p_part[0, lo] + (p_in[3] + p_in[4])) + bias).astype(BF16).astype(F32)
    y_all[x, mine, hi] = (x1_all[mine, hi] + (p_part[0, hi] + (p_in[2] + p_in[5])) + bias).astype(BF16).astype(F32)

    def unit(dx, dy, rows=every, at=all_cols):
        return y_all.at[lax.rem(x + dx, n), c * n + lax.rem(y + dy, n), rows, at]

    def relay(dx, dy, dev, rows=every, at=all_cols):
        ref = unit(dx, dy, rows, at)
        return push(ref, ref, dev)

    fwd = []

    def forward(dx, dy):
        fwd.append(relay(dx, dy, partner))

    xp, xm, yp, ym = along_x(1), along_x(3), along_y(1), along_y(3)
    own = {}
    for first_half in (True, False):
        for key, dev in (("xp", xp), ("xm", xm), ("yp", yp), ("ym", ym)):
            own[key, first_half] = relay(0, 0, dev, at=left if (key[1] == "p") == first_half else right)
    forward(0, 0)
    own["xp", True].wait_recv()
    r_xp = relay(3, 0, xp, at=left)
    own["xm", True].wait_recv()
    r_xm = relay(1, 0, xm, at=right)
    own["yp", True].wait_recv()
    r_yp = relay(0, 3, yp, at=left)
    own["ym", True].wait_recv()
    r_ym = relay(0, 1, ym, at=right)
    own["xp", False].wait_recv()
    a_yp, a_ym = relay(3, 0, yp, rows=lo), relay(3, 0, ym, rows=lo)
    own["xm", False].wait_recv()
    b_yp, b_ym = relay(1, 0, yp, rows=lo), relay(1, 0, ym, rows=lo)
    own["yp", False].wait_recv()
    a_xp, a_xm = relay(0, 3, xp, rows=hi), relay(0, 3, xm, rows=hi)
    own["ym", False].wait_recv()
    b_xp, b_xm = relay(0, 1, xp, rows=hi), relay(0, 1, xm, rows=hi)
    for d in ((3, 0), (1, 0), (0, 3), (0, 1)):
        forward(*d)
    r_xp.wait_recv()
    c_yp, c_ym = relay(2, 0, yp, lo, left), relay(2, 0, ym, lo, left)
    r_xm.wait_recv()
    d_yp, d_ym = relay(2, 0, yp, lo, right), relay(2, 0, ym, lo, right)
    r_yp.wait_recv()
    c_xp, c_xm = relay(0, 2, xp, hi, left), relay(0, 2, xm, hi, left)
    r_ym.wait_recv()
    d_xp, d_xm = relay(0, 2, xp, hi, right), relay(0, 2, xm, hi, right)
    forward(2, 0)
    forward(0, 2)
    late = []
    for cp, dx, dy, dev, rows, at in ((a_yp, 3, 3, yp, lo, left), (a_ym, 3, 1, ym, lo, right),
                                      (b_yp, 1, 3, yp, lo, left), (b_ym, 1, 1, ym, lo, right),
                                      (a_xp, 3, 3, xp, hi, left), (a_xm, 1, 3, xm, hi, right),
                                      (b_xp, 3, 1, xp, hi, left), (b_xm, 1, 1, xm, hi, right)):
        cp.wait_recv()
        late.append(relay(dx, dy, dev, rows, at))
    for d in ((3, 3), (3, 1), (1, 3), (1, 1)):
        forward(*d)
    for cp, dx, dy, dev, rows, at in ((c_yp, 2, 3, yp, lo, left), (d_ym, 2, 1, ym, lo, right),
                                      (c_xp, 3, 2, xp, hi, left), (d_xm, 1, 2, xm, hi, right)):
        cp.wait_recv()
        late.append(relay(dx, dy, dev, rows, at))
    for cp in (c_ym, d_yp, c_xm, d_xp):
        cp.wait_recv()
    for cp in late[:8]:
        cp.wait_recv()
    for d in ((3, 2), (1, 2), (2, 3), (2, 1)):
        forward(*d)
    for cp in late[8:]:
        cp.wait_recv()
    forward(2, 2)
    for cp in fwd:
        cp.wait_recv()
    for s in range(steps):
        for xb in range(0, n, 2):
            for i in range(2 * n):
                block = jnp.concatenate([y_all[xb, i, s * blk_b:(s + 1) * blk_b, :],
                                         y_all[xb + 1, i, s * blk_b:(s + 1) * blk_b, :]], axis=0)
                y_ref[s, xb * blk_b:(xb + 2) * blk_b, i * cols:(i + 1) * cols] = block.astype(BF16)
    for cp in sent:
        cp.wait_send()


def copy_kernel(src, dst, buf, in_sem, out_sem):
    for i in range(buf.shape[0]):
        pltpu.make_async_copy(src.at[i], buf.at[i], in_sem.at[i]).start()
    for i in range(buf.shape[0]):
        pltpu.make_async_copy(src.at[i], buf.at[i], in_sem.at[i]).wait()
        pltpu.make_async_copy(buf.at[i], dst.at[i], out_sem.at[i]).start()
    for i in range(buf.shape[0]):
        pltpu.make_async_copy(buf.at[i], dst.at[i], out_sem.at[i]).wait()


def solution(mesh):
    n_sq = mesh.shape["sq"]
    n_y = mesh.shape["tp"]
    n_x = n_sq // 2
    act_spec = P(None, "dp", None)
    cache_spec = P("dp", "sq", "tp", None)
    col_spec = P(None, "tp")
    row_spec = P("tp", None)
    vec_spec = P("tp")
    rep_spec = P(None)
    in_specs = (act_spec, P("dp"), cache_spec, cache_spec, col_spec, vec_spec, col_spec, vec_spec,
                col_spec, vec_spec, row_spec, rep_spec, rep_spec, rep_spec, rep_spec, rep_spec,
                col_spec, vec_spec, row_spec, rep_spec)
    out_specs = (act_spec, cache_spec, cache_spec)
    vmem = pl.BlockSpec(memory_space=pltpu.VMEM)
    hbm = pl.BlockSpec(memory_space=pl.ANY)

    def per_device(x_steps, positions, key_buf, val_buf, w_q, b_q, w_k, b_k, w_v, b_v, w_o, b_o,
                   ln1_gain, ln1_bias, ln2_gain, ln2_bias, w_fc, b_fc, w_proj, b_proj):
        steps, batch, width = x_steps.shape
        local, head_dim = key_buf.shape[1], key_buf.shape[3]
        rows = steps * batch
        heads = w_q.shape[1] // head_dim
        half = heads // 2
        half_dim = head_dim // 2
        inv_freq = jnp.power(jnp.float32(ROPE_BASE), -2.0 * jnp.arange(half_dim, dtype=F32) / head_dim)
        inv_freq = jnp.concatenate([inv_freq, inv_freq])[None, None, :]
        sign = jnp.where(jnp.arange(head_dim) < half_dim, -1.0, 1.0).astype(F32)
        shape = (steps, batch, head_dim)
        cur = jnp.broadcast_to(positions[None, :, None], shape) + lax.broadcasted_iota(jnp.int32, shape, 0)
        angle = cur.astype(F32) * inv_freq
        cos_t = jnp.cos(angle).reshape(rows, head_dim)
        sin_t = (jnp.sin(angle) * sign).reshape(rows, head_dim)

        per, bands = 8, 6
        groups = batch // per
        smem = pl.BlockSpec(memory_space=pltpu.SMEM)
        part, k_new, v_new = pl.pallas_call(
            functools.partial(front_kernel, batch=batch, heads=heads, head_dim=head_dim, steps=steps, per=per),
            out_shape=(jax.ShapeDtypeStruct((2, half + 1, rows, head_dim), F32),
                       jax.ShapeDtypeStruct((batch, local, head_dim), BF16),
                       jax.ShapeDtypeStruct((batch, local, head_dim), BF16)),
            in_specs=[smem] + [hbm] * 4 + [vmem] * 7 + [hbm] * 2,
            out_specs=(vmem, hbm, hbm),
            scratch_shapes=[
                pltpu.VMEM((rows, width), BF16),
                pltpu.VMEM((rows, width), BF16),
                pltpu.VMEM((bands, width // bands, heads * head_dim), BF16),
                pltpu.VMEM((width, head_dim), BF16),
                pltpu.VMEM((width, head_dim), BF16),
                pltpu.VMEM((rows, heads * head_dim), F32),
                pltpu.VMEM((heads + 2, rows, head_dim), F32),
                pltpu.VMEM((batch, local, head_dim), BF16),
                pltpu.VMEM((batch, local, head_dim), BF16),
                pltpu.VMEM((per // 2, heads, 2 * steps, local), F32),
                pltpu.VMEM((per // 2, heads, 2 * steps, head_dim), F32),
                pltpu.VMEM((per // 2, heads * 2 * steps, local + head_dim), BF16),
                pltpu.SemaphoreType.DMA((rows // 16,)),
                pltpu.SemaphoreType.DMA((bands,)),
                pltpu.SemaphoreType.DMA((2,)),
                pltpu.SemaphoreType.DMA((2, groups)),
                pltpu.SemaphoreType.DMA((2, groups)),
            ],
            compiler_params=pltpu.CompilerParams(vmem_limit_bytes=VMEM_BYTES),
            name="front",
        )(positions, x_steps.reshape(rows, width), w_q, w_k, w_v, ln1_gain, ln1_bias, b_q, b_k, b_v, cos_t, sin_t,
          key_buf.reshape(batch, local, head_dim), val_buf.reshape(batch, local, head_dim))

        cols = width // (2 * n_y)
        core_cols = width // 2
        blk_b = batch // n_x
        blk = blk_b * steps
        ys = pl.pallas_call(
            functools.partial(tail_kernel, half=half, head_dim=head_dim),
            out_shape=jax.ShapeDtypeStruct((steps, batch, width), BF16),
            in_specs=[vmem, hbm] + [vmem] * 5 + [hbm] * 3,
            out_specs=vmem,
            scratch_shapes=[
                pltpu.VMEM((5, width, cols), BF16),
                pltpu.VMEM((steps, blk_b, cols), BF16),
                pltpu.VMEM((4, half + 1, blk, head_dim), F32),
                pltpu.VMEM((4, half + 1, blk, head_dim), F32),
                pltpu.VMEM((6, half + 1, blk // 2, head_dim), F32),
                pltpu.VMEM((blk, half * head_dim), F32),
                pltpu.VMEM((blk, half * head_dim), F32),
                pltpu.VMEM((blk, heads * head_dim), BF16),
                pltpu.VMEM((4, blk, cols), F32),
                pltpu.VMEM((6, blk // 2, cols), F32),
                pltpu.VMEM((8, blk, cols), F32),
                pltpu.VMEM((blk, width), BF16),
                pltpu.VMEM((4, blk, cols), F32),
                pltpu.VMEM((4, blk, cols), F32),
                pltpu.VMEM((blk, w_proj.shape[0]), BF16),
                pltpu.VMEM((4, blk, cols), F32),
                pltpu.VMEM((6, blk // 2, cols), F32),
                pltpu.VMEM((4, 8, blk, cols), F32),
                pltpu.VMEM((40, width), F32),
                pltpu.VMEM((w_proj.shape[0], cols // 2), BF16),
                pltpu.SemaphoreType.DMA((13,)),
                pltpu.SemaphoreType.DMA,
                pltpu.SemaphoreType.DMA((100,)),
                pltpu.SemaphoreType.DMA((100,)),
            ],
            compiler_params=pltpu.CompilerParams(collective_id=0, has_side_effects=True, vmem_limit_bytes=VMEM_BYTES),
            name="tail",
        )(part, x_steps, b_o, b_proj, ln2_gain, ln2_bias, b_fc, w_o, w_fc, w_proj)
        ys = pl.pallas_call(
            copy_kernel,
            out_shape=jax.ShapeDtypeStruct(ys.shape, ys.dtype),
            in_specs=[hbm],
            out_specs=hbm,
            scratch_shapes=[pltpu.VMEM(ys.shape, ys.dtype), pltpu.SemaphoreType.DMA((steps,)), pltpu.SemaphoreType.DMA((steps,))],
            name="ys_copy",
        )(ys)
        return ys, k_new.reshape(key_buf.shape), v_new.reshape(val_buf.shape)

    return jax.shard_map(per_device, mesh=mesh, in_specs=in_specs, out_specs=out_specs, check_vma=False)
```

```python
import functools

import jax
import jax.numpy as jnp
from jax import lax
from jax.experimental import pallas as pl
from jax.experimental.pallas import tpu as pltpu
from jax.sharding import PartitionSpec as P

ROPE_BASE = 1000000.0
LN_EPS = 1e-5
NEG_BIG = -1e30
MESH = pl.DeviceIdType.MESH
F32 = jnp.float32
BF16 = jnp.bfloat16
VMEM_BYTES = 67043328


def one_hot_rows(size, inner):
    outer = size // inner
    row = lax.broadcasted_iota(jnp.int32, (size, size), 0)
    col = lax.broadcasted_iota(jnp.int32, (size, size), 1)
    source = lax.rem(row, outer) * inner + lax.div(row, outer)
    return jnp.where(col == source, 1.0, 0.0).astype(BF16)


def front_kernel(pos_ref, x_any, wq_any, wk_any, wv_any, gain_any, shift_any, bq_any, bk_any, bv_any, cos_any, sin_any,
                 kc_any, vc_any,
                 part_ref, kout_any, vout_any,
                 x_buf, hid, wq_buf, wk_buf, wv_buf, acc, qkv, k_buf, v_buf, s_buf, n_buf, p_buf,
                 gain_ref, shift_ref, bq_ref, bk_ref, bv_ref, cos_ref, sin_ref, par_sem,
                 x_sem, wq_sem, kv_sem, c_sem, out_sem, *, batch, heads, head_dim, steps, per):
    rows, width = x_buf.shape
    n_q = heads * head_dim
    bands, band = wq_buf.shape[0], wq_buf.shape[1]
    local = k_buf.shape[1]
    slots = local * lax.axis_size("sq")
    groups = batch // per
    half = heads // 2
    first = lax.axis_index("sq") * local
    leader = lax.axis_index("sq") == 0

    def x_copy(i):
        at = pl.ds(pl.multiple_of(i * 16, 16), 16)
        return pltpu.make_async_copy(x_any.at[at], x_buf.at[at], x_sem.at[i])

    params = [pltpu.make_async_copy(src, dst, par_sem.at[i]) for i, (src, dst) in enumerate(
        ((gain_any, gain_ref), (shift_any, shift_ref), (bq_any, bq_ref), (bk_any, bk_ref), (bv_any, bv_ref),
         (cos_any, cos_ref), (sin_any, sin_ref)))]
    x_copy(0).start()
    for cp in params:
        cp.start()
    for i in range(1, rows // 16):
        x_copy(i).start()
    k_copy = pltpu.make_async_copy(wk_any, wk_buf, kv_sem.at[0])
    v_copy = pltpu.make_async_copy(wv_any, wv_buf, kv_sem.at[1])

    def q_copy(i):
        return pltpu.make_async_copy(wq_any.at[pl.ds(pl.multiple_of(i * band, band), band), :], wq_buf.at[i], wq_sem.at[i])

    def cache_in(i):
        at = pl.ds(i * per, per)
        return (pltpu.make_async_copy(kc_any.at[at], k_buf.at[at], c_sem.at[0, i]),
                pltpu.make_async_copy(vc_any.at[at], v_buf.at[at], c_sem.at[1, i]))

    def cache_out(i):
        at = pl.ds(i * per, per)
        return (pltpu.make_async_copy(k_buf.at[at], kout_any.at[at], out_sem.at[0, i]),
                pltpu.make_async_copy(v_buf.at[at], vout_any.at[at], out_sem.at[1, i]))

    k_copy.start()
    v_copy.start()
    q_copy(0).start()
    for cp in params:
        cp.wait()
    gain = as_row(gain_ref)
    shift = as_row(shift_ref)

    def norm_rows(i, carry):
        x_copy(i).wait()
        at = pl.ds(pl.multiple_of(i * 16, 16), 16)
        vals = x_buf[at, :].astype(F32)
        mean = jnp.sum(vals, axis=-1, keepdims=True) * (1.0 / width)
        vals = vals - mean
        var = jnp.sum(vals * vals, axis=-1, keepdims=True) * (1.0 / width)
        hid[at, :] = (vals * lax.rsqrt(var + LN_EPS) * gain + shift).astype(BF16)
        return carry

    lax.fori_loop(0, rows // 16, norm_rows, 0, unroll=2)
    for i in range(1, bands // 2):
        q_copy(i).start()

    perm = one_hot_rows(rows, batch)
    cos_t = cos_ref[...]
    sin_t = sin_ref[...]

    def rotate(vals):
        return vals * cos_t + pltpu.roll(vals, head_dim // 2, 1) * sin_t

    def by_batch(vals):
        return jnp.dot(perm, vals.astype(BF16), preferred_element_type=F32)

    k_copy.wait()
    v_copy.wait()
    for i in range(bands // 2, bands):
        q_copy(i).start()
    k_new = jnp.dot(hid[...], wk_buf[...], preferred_element_type=F32) + as_row(bk_ref)
    v_new = jnp.dot(hid[...], wv_buf[...], preferred_element_type=F32) + as_row(bv_ref)
    qkv[heads] = by_batch(rotate(k_new.astype(BF16).astype(F32)))
    qkv[heads + 1] = by_batch(v_new)
    acc[...] = jnp.broadcast_to(as_row(bq_ref), acc.shape)

    def q_band(i, carry):
        q_copy(i).wait()

        @pl.when(i >= bands - groups // 2)
        def _():
            for j in range(2):
                for cp in cache_in(2 * (i - bands + groups // 2) + j):
                    cp.start()

        acc[...] += jnp.dot(hid[:, pl.ds(pl.multiple_of(i * band, band), band)], wq_buf[i], preferred_element_type=F32)
        return carry

    lax.fori_loop(0, bands, q_band, 0)

    for h in range(heads):
        vals = acc[:, h * head_dim:(h + 1) * head_dim]
        qkv[h] = by_batch(rotate(vals.astype(BF16).astype(F32)))

    scale = head_dim ** -0.5
    pair_rows = 2 * steps
    row = lax.broadcasted_iota(jnp.int32, (pair_rows, local), 0)
    slot = lax.broadcasted_iota(jnp.int32, (pair_rows, local), 1) + first
    step = lax.rem(row, steps)
    n_row = lax.broadcasted_iota(jnp.int32, (pair_rows, head_dim), 0)
    n_col = lax.broadcasted_iota(jnp.int32, (pair_rows, head_dim), 1)
    new_ok = ((lax.div(n_row, steps) == lax.div(n_col, steps)) & (lax.rem(n_col, steps) <= lax.rem(n_row, steps))
              & (n_col < pair_rows) & leader)[None]
    lane = n_col
    pad = jnp.zeros((head_dim - pair_rows, head_dim), F32)
    window = lax.broadcasted_iota(jnp.int32, (16, head_dim), 0)
    nt = (((1,), (1,)), ((), ()))

    def group(i, carry):
        for cp in cache_in(i):
            cp.wait()
        s_shape = (heads, pair_rows, local)
        o_shape = (heads, pair_rows, head_dim)

        def rows_of(pr):
            return pl.ds(pl.multiple_of(i * (per * steps) + pair_rows * pr, pair_rows), pair_rows)

        def mask_of(pr):
            b0 = i * per + 2 * pr
            cur = jnp.where(row < steps, pos_ref[b0], pos_ref[b0 + 1]) + step
            if slots & (slots - 1):
                dist = lax.rem(lax.rem(cur - slot, slots) + slots, slots)
            else:
                dist = (cur - slot) & (slots - 1)
            return ((dist > step) & (dist <= cur))[None]

        for pr in range(per // 2):
            b0 = i * per + 2 * pr
            query = qkv[0:heads, rows_of(pr), :].reshape(heads * pair_rows, head_dim).astype(BF16)
            new_k = jnp.concatenate([qkv[heads, rows_of(pr), :], pad], axis=0).astype(BF16)
            score0 = lax.dot_general(query, k_buf[b0], nt, preferred_element_type=F32).reshape(s_shape)
            score1 = lax.dot_general(query, k_buf[b0 + 1], nt, preferred_element_type=F32).reshape(s_shape)
            s_buf[pr] = jnp.where(mask_of(pr), jnp.where((row < steps)[None], score0, score1) * scale, NEG_BIG)
            score_n = lax.dot_general(query, new_k, nt, preferred_element_type=F32).reshape(o_shape) * scale
            n_buf[pr] = jnp.where(new_ok, score_n, NEG_BIG)
        for pr in range(per // 2):
            score = s_buf[pr]
            score_n = n_buf[pr]
            top = jnp.max(jnp.maximum(score_n, functools.reduce(
                jnp.maximum, [score[:, :, j:j + head_dim] for j in range(0, local, head_dim)])), axis=-1, keepdims=True)
            wts = jnp.where(mask_of(pr), jnp.exp(score - top), 0.0)
            wts_n = jnp.where(new_ok, jnp.exp(score_n - top), 0.0)
            total = jnp.sum(wts_n + sum(wts[:, :, j:j + head_dim] for j in range(0, local, head_dim)), axis=-1, keepdims=True)
            p_buf[pr, :, 0:local] = wts.reshape(heads * pair_rows, local).astype(BF16)
            p_buf[pr, :, local:] = wts_n.reshape(heads * pair_rows, head_dim).astype(BF16)
            for core in range(2):
                stat = jnp.zeros((pair_rows, head_dim), F32)
                for h in range(half):
                    stat = jnp.where(lane == h, top[core * half + h], stat)
                    stat = jnp.where(lane == head_dim // 2 + h, total[core * half + h], stat)
                part_ref[core, half, rows_of(pr), :] = stat
        for pr in range(per // 2):
            b0 = i * per + 2 * pr
            new_v = jnp.concatenate([qkv[heads + 1, rows_of(pr), :], pad], axis=0).astype(BF16)
            out0 = jnp.dot(p_buf[pr, :, 0:local], v_buf[b0], preferred_element_type=F32).reshape(o_shape)
            out1 = jnp.dot(p_buf[pr, :, 0:local], v_buf[b0 + 1], preferred_element_type=F32).reshape(o_shape)
            out_n = jnp.dot(p_buf[pr, :, local:], new_v, preferred_element_type=F32).reshape(o_shape)
            out = jnp.where((n_row < steps)[None], out0, out1) + out_n
            for core in range(2):
                part_ref[core, 0:half, rows_of(pr), :] = out[core * half:(core + 1) * half]
        for b in range(per):
            lead = pos_ref[i * per + b] - first
            head_at = lax.rem(lead + slots, slots)

            @pl.when((head_at < local) | (head_at >= slots - steps))
            def _(b=b, head_at=head_at):
                for t in range(steps):
                    at = lax.rem(head_at + t, slots)

                    @pl.when(at < local)
                    def _(t=t, at=at):
                        start = pl.multiple_of(lax.div(at, 16) * 16, 16)
                        hit = window == at - start
                        for src, dst in ((heads, k_buf), (heads + 1, v_buf)):
                            fresh = qkv[src, pl.ds(i * (per * steps) + b * steps + t, 1), :]
                            old = dst[i * per + b, pl.ds(start, 16), :].astype(F32)
                            dst[i * per + b, pl.ds(start, 16), :] = jnp.where(hit, fresh, old).astype(BF16)

        for cp in cache_out(i):
            cp.start()
        return carry

    lax.fori_loop(0, groups, group, 0)
    for i in range(groups):
        for cp in cache_out(i):
            cp.wait()


def as_row(ref):
    return ref[...].astype(F32).reshape(1, ref.shape[0])


def merge_parts(parts, half, head_dim):
    stats = [p[half] for p in parts]
    top = functools.reduce(jnp.maximum, stats)
    scales = [jnp.exp(s - top) for s in stats]
    lane = lax.broadcasted_iota(jnp.int32, top.shape, 1)
    total = sum(s * pltpu.roll(f, head_dim // 2, 1) for s, f in zip(stats, scales))
    stat = jnp.where(lane < head_dim // 2, top, total)
    outs = []
    for h in range(half):
        outs.append(sum(p[h] * f[:, h:h + 1] for p, f in zip(parts, scales)))
    return outs, stat


def tail_kernel(part_any, x_any, bo_any, bpj_any, gain_any, shift_any, bfc_any, wo_any, wfc_any, wpj_any, y_ref,
                w_buf, x_buf, pair_in, m_part, x_in, a_own, a_in, a_full, o_part, o_in, x1_all, hid,
                g_own, g_in, g_full, p_part, p_in, y_all, bias_rows, w_ext, part_ref, bo_ref, bpj_ref, gain_ref, shift_ref, bfc_ref, par_sem, w_sem, x_sem, send, recv, *, half, head_dim):
    steps, blk_b, cols = x_buf.shape
    blk = steps * blk_b
    n = 4
    width = 2 * n * cols
    core_cols = n * cols
    depth = wo_any.shape[0]
    ff = wpj_any.shape[0]
    sq = lax.axis_index("sq")
    y = lax.axis_index("tp")
    x = lax.div(sq, 2)
    c = lax.rem(sq, 2)
    mine = c * n + y
    my_col = pl.multiple_of(mine * cols, cols)
    half_col = pl.multiple_of(c * core_cols, core_cols)
    lo, hi = pl.ds(0, blk // 2), pl.ds(blk // 2, blk // 2)
    left, right = pl.ds(0, cols // 2), pl.ds(cols // 2, cols // 2)
    every = pl.ds(0, blk)
    all_cols = pl.ds(0, cols)
    partner = {"tp": y, "sq": 2 * x + 1 - c}

    def along_x(d):
        return {"tp": y, "sq": 2 * lax.rem(x + d, n) + c}

    def along_y(d):
        return {"tp": lax.rem(y + d, n), "sq": sq}

    ids = iter(range(1000))
    sent = []

    def push(src, dst, dev):
        i = next(ids)
        cp = pltpu.make_async_remote_copy(src_ref=src, dst_ref=dst, send_sem=send.at[i], recv_sem=recv.at[i],
                                          device_id=dev, device_id_type=MESH)
        cp.start()
        sent.append(cp)
        return cp

    order = (2, 1, 3, 0)

    def block_col(d):
        return pl.multiple_of(half_col + lax.rem(y + d, n) * cols, cols)

    wo_copy = [pltpu.make_async_copy(wo_any.at[:, pl.ds(block_col(d), cols)], w_buf.at[0, pl.ds(d * depth, depth)], w_sem.at[d])
               for d in range(n)]
    fc_copy = [pltpu.make_async_copy(wfc_any.at[:, pl.ds(pl.multiple_of(half_col + j * cols, cols), cols)], w_buf.at[1 + j],
                                     w_sem.at[n + j]) for j in range(n)]
    pj_copy = [pltpu.make_async_copy(wpj_any.at[:, pl.ds(block_col(d), cols)], w_buf.at[k], w_sem.at[2 * n + k])
               for k, d in enumerate(order)]
    hc = cols // 2
    pj_copy[1] = pltpu.make_async_copy(wpj_any.at[:, pl.ds(pl.multiple_of(block_col(1) + hc, hc), hc)], w_buf.at[1, :, pl.ds(0, hc)],
                                       w_sem.at[2 * n + 1])
    ext_copy = pltpu.make_async_copy(wpj_any.at[:, pl.ds(block_col(1), hc)], w_ext, w_sem.at[3 * n])
    x_copy = pltpu.make_async_copy(x_any.at[:, pl.ds(pl.multiple_of(x * blk_b, blk_b), blk_b), pl.ds(my_col, cols)], x_buf, x_sem)
    params = [pltpu.make_async_copy(src, dst, par_sem.at[i]) for i, (src, dst) in enumerate(
        ((part_any, part_ref), (bo_any, bo_ref), (bpj_any, bpj_ref), (gain_any, gain_ref), (shift_any, shift_ref),
         (bfc_any, bfc_ref)))]
    for cp in params:
        cp.start()
    x_copy.start()
    for d in order:
        wo_copy[d].start()

    barrier = pltpu.get_barrier_semaphore()
    peers = [partner] + [along_x(d) for d in (1, 3)] + [along_y(d) for d in (1, 3)]
    for dev in peers:
        pl.semaphore_signal(barrier, inc=1, device_id=dev, device_id_type=MESH)
    for cp in params:
        cp.wait()
    for i, ref in enumerate((bo_ref, bpj_ref, bfc_ref, gain_ref, shift_ref)):
        bias_rows[8 * i:8 * i + 1, :] = as_row(ref)
    pl.semaphore_wait(barrier, len(peers))

    def ring_reduce(ready, half_of, inbox, along, fold):
        ready(2)
        rel_a = push(half_of(2, lo), inbox.at[0], along(1))
        rel_b = push(half_of(2, hi), inbox.at[1], along(3))
        ready(1)
        dir_b = push(half_of(1, hi), inbox.at[2], along(1))
        ready(3)
        dir_a = push(half_of(3, lo), inbox.at[3], along(3))
        rel_a.wait_recv()
        fold(1, lo, 0)
        sum_a = push(half_of(1, lo), inbox.at[4], along(1))
        rel_b.wait_recv()
        fold(3, hi, 1)
        sum_b = push(half_of(3, hi), inbox.at[5], along(3))
        ready(0)
        for cp in (dir_b, dir_a, sum_a, sum_b):
            cp.wait_recv()

    planes = range(half + 1)
    pairs = {}
    for d in order:
        at = pl.ds(pl.multiple_of(lax.rem(x + d, n) * blk, blk), blk)
        pairs[d] = push(part_ref.at[1 - c, :, at, :], pair_in.at[d], partner)
    fc_copy[0].start()
    fc_copy[1].start()

    def pair_merge(d):
        pairs[d].wait_recv()
        at = pl.ds(pl.multiple_of(lax.rem(x + d, n) * blk, blk), blk)
        outs, stat = merge_parts([[part_ref[c, h, at, :] for h in planes], [pair_in[d, h] for h in planes]], half, head_dim)
        for h in range(half):
            m_part[d, h] = outs[h]
        m_part[d, half] = stat

    def fold_parts(d, rows, i):
        outs, stat = merge_parts([[m_part[d, h, rows, :] for h in planes], [x_in[i, h] for h in planes]], half, head_dim)
        for h in range(half):
            m_part[d, h, rows, :] = outs[h]
        m_part[d, half, rows, :] = stat

    ring_reduce(pair_merge, lambda d, rows: m_part.at[d, :, rows], x_in, along_x, fold_parts)
    for rows, terms in ((lo, (3, 4)), (hi, (2, 5))):
        parts = [[m_part[0, h, rows, :] for h in planes]] + [[x_in[i, h] for h in planes] for i in terms]
        outs, stat = merge_parts(parts, half, head_dim)
        for h in range(half):
            denom = stat[:, head_dim // 2 + h:head_dim // 2 + h + 1]
            a_own[rows, h * head_dim:(h + 1) * head_dim] = (outs[h] / denom).astype(BF16).astype(F32)
    a_copy = push(a_own, a_in, partner)
    fc_copy[2].start()
    fc_copy[3].start()
    perm = one_hot_rows(blk, steps)
    a_cols = half * head_dim
    a_full[:, pl.ds(pl.multiple_of(c * a_cols, a_cols), a_cols)] = jnp.dot(
        perm, a_own[...].astype(BF16), preferred_element_type=F32).astype(BF16)
    a_copy.wait_recv()
    a_full[:, pl.ds(pl.multiple_of((1 - c) * a_cols, a_cols), a_cols)] = jnp.dot(
        perm, a_in[...].astype(BF16), preferred_element_type=F32).astype(BF16)

    def o_block(d):
        wo_copy[d].wait()
        o_part[d] = jnp.dot(a_full[...], w_buf[0, d * depth:(d + 1) * depth, :], preferred_element_type=F32)

    def fold_o(d, rows, i):
        o_part[d, rows, :] = o_part[d, rows, :] + o_in[i]

    ring_reduce(o_block, lambda d, rows: o_part.at[d, rows], o_in, along_y, fold_o)
    pj_copy[0].start()
    ext_copy.start()
    x_copy.wait()
    x_own = x_buf[...].astype(F32).reshape(blk, cols) + bias_rows[0:1, pl.ds(my_col, cols)]
    hb = blk // 2
    x1_all[mine, lo] = (x_own[:hb] + (o_part[0, lo] + (o_in[3] + o_in[4]))).astype(BF16).astype(F32)
    x1_all[mine, hi] = (x_own[hb:] + (o_part[0, hi] + (o_in[2] + o_in[5]))).astype(BF16).astype(F32)

    def x1_push(d, rows, dev):
        ref = x1_all.at[c * n + lax.rem(y + d, n), rows]
        return push(ref, ref, dev)

    p_lo = x1_push(0, lo, along_y(1))
    m_hi = x1_push(0, hi, along_y(3))
    p_hi = x1_push(0, hi, along_y(1))
    m_lo = x1_push(0, lo, along_y(3))
    fwd = [x1_push(0, every, partner)]
    p_lo.wait_recv()
    r_lo = x1_push(3, lo, along_y(1))
    m_hi.wait_recv()
    r_hi = x1_push(1, hi, along_y(3))
    p_hi.wait_recv()
    fwd.append(x1_push(3, every, partner))
    m_lo.wait_recv()
    fwd.append(x1_push(1, every, partner))
    r_lo.wait_recv()
    r_hi.wait_recv()
    fwd.append(x1_push(2, every, partner))
    for cp in fwd:
        cp.wait_recv()

    total = jnp.zeros((blk, 1), F32)
    for i in range(2 * n):
        total = total + jnp.sum(x1_all[i], axis=-1, keepdims=True)
    mean = total * (1.0 / width)
    total = jnp.zeros((blk, 1), F32)
    for i in range(2 * n):
        dev = x1_all[i] - mean
        total = total + jnp.sum(dev * dev, axis=-1, keepdims=True)
    inv = lax.rsqrt(total * (1.0 / width) + LN_EPS)
    for i in range(2 * n):
        at = slice(i * cols, (i + 1) * cols)
        gain = bias_rows[24:25, at]
        shift = bias_rows[32:33, at]
        hid[:, at] = ((x1_all[i] - mean) * inv * gain + shift).astype(BF16)

    own_ff = pl.multiple_of(c * (ff // 2), ff // 2)
    g_copy = []
    for j in range(n):
        fc_copy[j].wait()

        val = jnp.dot(hid[...], w_buf[1 + j], preferred_element_type=F32)
        ff_at = pl.ds(pl.multiple_of(own_ff + j * cols, cols), cols)
        val = jax.nn.gelu(val + bias_rows[16:17, ff_at], approximate=True).astype(BF16)
        g_own[j] = val.astype(F32)
        g_full[:, ff_at] = val
        g_copy.append(push(g_own.at[j], g_in.at[j], partner))
        if j < n - 1:
            pj_copy[j + 1].start()
    other_ff = pl.multiple_of((1 - c) * (ff // 2), ff // 2)

    def p_block(d):
        k = order.index(d)
        pj_copy[k].wait()
        if k == 0:
            own_rows, other_rows = pl.ds(own_ff, ff // 2), pl.ds(other_ff, ff // 2)
            p_part[d] = jnp.dot(g_full[:, own_rows], w_buf[k, own_rows, :], preferred_element_type=F32)
            for j in range(n):
                g_copy[j].wait_recv()
                g_full[:, pl.ds(pl.multiple_of(other_ff + j * cols, cols), cols)] = g_in[j].astype(BF16)
            p_part[d] = p_part[d] + jnp.dot(g_full[:, other_rows], w_buf[k, other_rows, :], preferred_element_type=F32)
        elif k == 1:
            ext_copy.wait()
            p_part[d, :, 0:hc] = jnp.dot(g_full[...], w_ext[...], preferred_element_type=F32)
            p_part[d, :, hc:] = jnp.dot(g_full[...], w_buf[k, :, 0:hc], preferred_element_type=F32)
        else:
            p_part[d] = jnp.dot(g_full[...], w_buf[k], preferred_element_type=F32)

    def fold_p(d, rows, i):
        p_part[d, rows, :] = p_part[d, rows, :] + p_in[i]

    ring_reduce(p_block, lambda d, rows: p_part.at[d, rows], p_in, along_y, fold_p)
    bias = bias_rows[8:9, pl.ds(my_col, cols)]
    y_all[x, mine, lo] = (x1_all[mine, lo] + (p_part[0, lo] + (p_in[3] + p_in[4])) + bias).astype(BF16).astype(F32)
    y_all[x, mine, hi] = (x1_all[mine, hi] + (p_part[0, hi] + (p_in[2] + p_in[5])) + bias).astype(BF16).astype(F32)

    def unit(dx, dy, rows=every, at=all_cols):
        return y_all.at[lax.rem(x + dx, n), c * n + lax.rem(y + dy, n), rows, at]

    def relay(dx, dy, dev, rows=every, at=all_cols):
        ref = unit(dx, dy, rows, at)
        return push(ref, ref, dev)

    fwd = []

    def forward(dx, dy):
        fwd.append(relay(dx, dy, partner))

    xp, xm, yp, ym = along_x(1), along_x(3), along_y(1), along_y(3)
    own = {}
    for first_half in (True, False):
        for key, dev in (("xp", xp), ("xm", xm), ("yp", yp), ("ym", ym)):
            own[key, first_half] = relay(0, 0, dev, at=left if (key[1] == "p") == first_half else right)
    forward(0, 0)
    step1 = (("xp", 3, 0, xp), ("xm", 1, 0, xm), ("yp", 0, 3, yp), ("ym", 0, 1, ym))
    ring, turn = {}, {}
    for first_half in (True, False):
        for key, dx, dy, dev in step1:
            own[key, first_half].wait_recv()
            at = left if (key[1] == "p") == first_half else right
            if first_half:
                ring[key] = relay(dx, dy, dev, at=at)
            rows = lo if dx else hi
            for other, turn_dev in ((("yp", yp), ("ym", ym)) if dx else (("xp", xp), ("xm", xm))):
                turn[key, other, at is left] = relay(dx, dy, turn_dev, rows, at)
    r_xp, r_xm, r_yp, r_ym = ring["xp"], ring["xm"], ring["yp"], ring["ym"]
    for d in ((3, 0), (1, 0), (0, 3), (0, 1)):
        forward(*d)
    r_xp.wait_recv()
    c_yp, c_ym = relay(2, 0, yp, lo, left), relay(2, 0, ym, lo, left)
    r_xm.wait_recv()
    d_yp, d_ym = relay(2, 0, yp, lo, right), relay(2, 0, ym, lo, right)
    r_yp.wait_recv()
    c_xp, c_xm = relay(0, 2, xp, hi, left), relay(0, 2, xm, hi, left)
    r_ym.wait_recv()
    d_xp, d_xm = relay(0, 2, xp, hi, right), relay(0, 2, xm, hi, right)
    forward(2, 0)
    forward(0, 2)
    late = []
    for key, dx, dy, dev in step1:
        rows = lo if dx else hi
        for other, turn_dev in ((("yp", yp), ("ym", ym)) if dx else (("xp", xp), ("xm", xm))):
            back = 3 if other[1] == "p" else 1
            on_left = other[1] == "p"
            turn[key, other, on_left].wait_recv()
            late.append(relay(dx or back, dy or back, turn_dev, rows, left if on_left else right))
    for key, dx, dy, dev in step1:
        for other in (("yp", "ym") if dx else ("xp", "xm")):
            turn[key, other, other[1] != "p"].wait_recv()
    for d in ((3, 3), (3, 1), (1, 3), (1, 1)):
        forward(*d)
    for cp, dx, dy, dev, rows, at in ((c_yp, 2, 3, yp, lo, left), (d_ym, 2, 1, ym, lo, right),
                                      (c_xp, 3, 2, xp, hi, left), (d_xm, 1, 2, xm, hi, right)):
        cp.wait_recv()
        late.append(relay(dx, dy, dev, rows, at))
    for cp in (c_ym, d_yp, c_xm, d_xp):
        cp.wait_recv()
    for cp in late[:8]:
        cp.wait_recv()
    for d in ((3, 2), (1, 2), (2, 3), (2, 1)):
        forward(*d)
    for cp in late[8:]:
        cp.wait_recv()
    forward(2, 2)
    for cp in fwd:
        cp.wait_recv()
    for s in range(steps):
        for xb in range(0, n, 2):
            for i in range(2 * n):
                block = jnp.concatenate([y_all[xb, i, s * blk_b:(s + 1) * blk_b, :],
                                         y_all[xb + 1, i, s * blk_b:(s + 1) * blk_b, :]], axis=0)
                y_ref[s, xb * blk_b:(xb + 2) * blk_b, i * cols:(i + 1) * cols] = block.astype(BF16)
    for cp in sent:
        cp.wait_send()


def copy_kernel(src, dst, buf, in_sem, out_sem):
    for i in range(buf.shape[0]):
        pltpu.make_async_copy(src.at[i], buf.at[i], in_sem.at[i]).start()
    for i in range(buf.shape[0]):
        pltpu.make_async_copy(src.at[i], buf.at[i], in_sem.at[i]).wait()
        pltpu.make_async_copy(buf.at[i], dst.at[i], out_sem.at[i]).start()
    for i in range(buf.shape[0]):
        pltpu.make_async_copy(buf.at[i], dst.at[i], out_sem.at[i]).wait()


def solution(mesh):
    n_sq = mesh.shape["sq"]
    n_y = mesh.shape["tp"]
    n_x = n_sq // 2
    act_spec = P(None, "dp", None)
    cache_spec = P("dp", "sq", "tp", None)
    col_spec = P(None, "tp")
    row_spec = P("tp", None)
    vec_spec = P("tp")
    rep_spec = P(None)
    in_specs = (act_spec, P("dp"), cache_spec, cache_spec, col_spec, vec_spec, col_spec, vec_spec,
                col_spec, vec_spec, row_spec, rep_spec, rep_spec, rep_spec, rep_spec, rep_spec,
                col_spec, vec_spec, row_spec, rep_spec)
    out_specs = (act_spec, cache_spec, cache_spec)
    vmem = pl.BlockSpec(memory_space=pltpu.VMEM)
    hbm = pl.BlockSpec(memory_space=pl.ANY)

    def per_device(x_steps, positions, key_buf, val_buf, w_q, b_q, w_k, b_k, w_v, b_v, w_o, b_o,
                   ln1_gain, ln1_bias, ln2_gain, ln2_bias, w_fc, b_fc, w_proj, b_proj):
        steps, batch, width = x_steps.shape
        local, head_dim = key_buf.shape[1], key_buf.shape[3]
        rows = steps * batch
        heads = w_q.shape[1] // head_dim
        half = heads // 2
        half_dim = head_dim // 2
        inv_freq = jnp.power(jnp.float32(ROPE_BASE), -2.0 * jnp.arange(half_dim, dtype=F32) / head_dim)
        inv_freq = jnp.concatenate([inv_freq, inv_freq])[None, None, :]
        sign = jnp.where(jnp.arange(head_dim) < half_dim, -1.0, 1.0).astype(F32)
        shape = (steps, batch, head_dim)
        cur = jnp.broadcast_to(positions[None, :, None], shape) + lax.broadcasted_iota(jnp.int32, shape, 0)
        angle = cur.astype(F32) * inv_freq
        cos_t = jnp.cos(angle).reshape(rows, head_dim)
        sin_t = (jnp.sin(angle) * sign).reshape(rows, head_dim)

        per, bands = 8, 6
        groups = batch // per
        smem = pl.BlockSpec(memory_space=pltpu.SMEM)
        part, k_new, v_new = pl.pallas_call(
            functools.partial(front_kernel, batch=batch, heads=heads, head_dim=head_dim, steps=steps, per=per),
            out_shape=(jax.ShapeDtypeStruct((2, half + 1, rows, head_dim), F32),
                       jax.ShapeDtypeStruct((batch, local, head_dim), BF16),
                       jax.ShapeDtypeStruct((batch, local, head_dim), BF16)),
            in_specs=[smem] + [hbm] * 13,
            out_specs=(vmem, hbm, hbm),
            scratch_shapes=[
                pltpu.VMEM((rows, width), BF16),
                pltpu.VMEM((rows, width), BF16),
                pltpu.VMEM((bands, width // bands, heads * head_dim), BF16),
                pltpu.VMEM((width, head_dim), BF16),
                pltpu.VMEM((width, head_dim), BF16),
                pltpu.VMEM((rows, heads * head_dim), F32),
                pltpu.VMEM((heads + 2, rows, head_dim), F32),
                pltpu.VMEM((batch, local, head_dim), BF16),
                pltpu.VMEM((batch, local, head_dim), BF16),
                pltpu.VMEM((per // 2, heads, 2 * steps, local), F32),
                pltpu.VMEM((per // 2, heads, 2 * steps, head_dim), F32),
                pltpu.VMEM((per // 2, heads * 2 * steps, local + head_dim), BF16),
                pltpu.VMEM((width,), BF16),
                pltpu.VMEM((width,), BF16),
                pltpu.VMEM((heads * head_dim,), BF16),
                pltpu.VMEM((head_dim,), BF16),
                pltpu.VMEM((head_dim,), BF16),
                pltpu.VMEM((rows, head_dim), F32),
                pltpu.VMEM((rows, head_dim), F32),
                pltpu.SemaphoreType.DMA((7,)),
                pltpu.SemaphoreType.DMA((rows // 16,)),
                pltpu.SemaphoreType.DMA((bands,)),
                pltpu.SemaphoreType.DMA((2,)),
                pltpu.SemaphoreType.DMA((2, groups)),
                pltpu.SemaphoreType.DMA((2, groups)),
            ],
            compiler_params=pltpu.CompilerParams(vmem_limit_bytes=VMEM_BYTES),
            name="front",
        )(positions, x_steps.reshape(rows, width), w_q, w_k, w_v, ln1_gain, ln1_bias, b_q, b_k, b_v, cos_t, sin_t,
          key_buf.reshape(batch, local, head_dim), val_buf.reshape(batch, local, head_dim))

        cols = width // (2 * n_y)
        core_cols = width // 2
        blk_b = batch // n_x
        blk = blk_b * steps
        ys = pl.pallas_call(
            functools.partial(tail_kernel, half=half, head_dim=head_dim),
            out_shape=jax.ShapeDtypeStruct((steps, batch, width), BF16),
            in_specs=[hbm] * 10,
            out_specs=vmem,
            scratch_shapes=[
                pltpu.VMEM((5, width, cols), BF16),
                pltpu.VMEM((steps, blk_b, cols), BF16),
                pltpu.VMEM((4, half + 1, blk, head_dim), F32),
                pltpu.VMEM((4, half + 1, blk, head_dim), F32),
                pltpu.VMEM((6, half + 1, blk // 2, head_dim), F32),
                pltpu.VMEM((blk, half * head_dim), F32),
                pltpu.VMEM((blk, half * head_dim), F32),
                pltpu.VMEM((blk, heads * head_dim), BF16),
                pltpu.VMEM((4, blk, cols), F32),
                pltpu.VMEM((6, blk // 2, cols), F32),
                pltpu.VMEM((8, blk, cols), F32),
                pltpu.VMEM((blk, width), BF16),
                pltpu.VMEM((4, blk, cols), F32),
                pltpu.VMEM((4, blk, cols), F32),
                pltpu.VMEM((blk, w_proj.shape[0]), BF16),
                pltpu.VMEM((4, blk, cols), F32),
                pltpu.VMEM((6, blk // 2, cols), F32),
                pltpu.VMEM((4, 8, blk, cols), F32),
                pltpu.VMEM((40, width), F32),
                pltpu.VMEM((w_proj.shape[0], cols // 2), BF16),
                pltpu.VMEM(part.shape, F32),
                pltpu.VMEM((width,), BF16),
                pltpu.VMEM((width,), BF16),
                pltpu.VMEM((width,), BF16),
                pltpu.VMEM((width,), BF16),
                pltpu.VMEM(b_fc.shape, BF16),
                pltpu.SemaphoreType.DMA((6,)),
                pltpu.SemaphoreType.DMA((13,)),
                pltpu.SemaphoreType.DMA,
                pltpu.SemaphoreType.DMA((112,)),
                pltpu.SemaphoreType.DMA((112,)),
            ],
            compiler_params=pltpu.CompilerParams(collective_id=0, has_side_effects=True, vmem_limit_bytes=VMEM_BYTES),
            name="tail",
        )(part, x_steps, b_o, b_proj, ln2_gain, ln2_bias, b_fc, w_o, w_fc, w_proj)
        ys = pl.pallas_call(
            copy_kernel,
            out_shape=jax.ShapeDtypeStruct(ys.shape, ys.dtype),
            in_specs=[hbm],
            out_specs=hbm,
            scratch_shapes=[pltpu.VMEM(ys.shape, ys.dtype), pltpu.SemaphoreType.DMA((steps,)), pltpu.SemaphoreType.DMA((steps,))],
            name="ys_copy",
        )(ys)
        return ys, k_new.reshape(key_buf.shape), v_new.reshape(val_buf.shape)

    return jax.shard_map(per_device, mesh=mesh, in_specs=in_specs, out_specs=out_specs, check_vma=False)
```
